32 devices in a mesh: seq: 4 (over z), head: 4 (over y, core), batch: 2 (over x).
Axes of the slice: x: 2, y: 2, z: 4, core: 2. Of those that a mesh axis runs over, the one named last changes fastest.
Arguments:
- tokens: bfloat16 [8192, 2048], P(('batch', 'seq')), parts along dimension 0, may hold values from -6 to 6
- neighbor_bank: bfloat16 [128, 256, 2048], P(('batch', 'seq')), parts along dimension 0, may hold values from -2100 to 2100
- slots: int32 [128], P(('batch', 'seq')), parts along dimension 0, may hold values from 0 to 15
- w_query: bfloat16 [2048, 2048], P('seq', 'head'), may hold values from -0.125 to 0.125
- w_key: bfloat16 [2048, 2048], P('seq', 'head'), may hold values from -0.125 to 0.125
- w_value: bfloat16 [2048, 2048], P('seq', 'head'), may hold values from -0.125 to 0.125
- w_out: bfloat16 [2048, 2048], P('head', 'seq'), may hold values from -0.125 to 0.125
Outputs:
- cross_out: bfloat16 [8192, 2048], P(('batch', 'seq'), 'head'), parts along dimension 0
The draws below stay inside these ranges and needn't reach their ends.
There are 2 independent parts, one for each index of `batch`. The reference program is written for one: setup_inputs(seed, part) draws one part's arguments, and reference() takes and returns one part's arrays. A program takes and returns all parts, laid end to end along the dimension named above; an argument that names none is the same for every part. Nothing has to cross between parts.
Inputs may be any that keep to these rules, and one draw needn't show every extreme that they name: Entry c picks row c // 16 * 16 + slots[c] of neighbor_bank.
All inputs are finite; a program needn't handle non-finite values.
Results may differ from the reference program's by a relative error of at most 0.006.
The reference program's roundings to bfloat16 on the way (of `normed`, `queries`, `retrieved`, `weights` and `attended`) count: a program that leaves them out, or rounds other values in their place, can miss the bound.
Values may be sent and summed in bfloat16 or wider, within the bound.
A program may use at most 128 MiB of HBM per device.

```python
import math
import jax
import jax.numpy as jnp
from jax import lax

D = 2048
HEADS = 16
HEAD_DIM = 128
BLOCK = 64
NEIGHBORS = 2
NEIGH_LEN = 128
BLOCK_DEV = 16
TOKENS = 4096
BLOCKS = 64


def draw_neighbor_bank(key, part):
    key_base = jax.random.fold_in(jax.random.fold_in(key, 11), 0)
    rows = NEIGHBORS * NEIGH_LEN
    base = jnp.clip(jax.random.normal(key_base, (BLOCKS, rows, D), jnp.float32) * 2.0, -8.0, 8.0)
    return base.astype(jnp.bfloat16)


def plant(drawn, own_key, low, largest):
    dims = drawn.shape
    spot = [jax.random.randint(jax.random.fold_in(own_key, axis), (), 0, dims[axis]) for axis in range(len(dims))]
    drawn = drawn.at[tuple(spot)].set(low)
    longest = dims.index(max(dims))
    spot[longest] = (spot[longest] + 1) % dims[longest]
    return drawn.at[tuple(spot)].set(largest)


def block_scale(rng, extent, cuts, smallest, high):
    def one(dim, parts):
        steps = jax.random.uniform(jax.random.fold_in(jax.random.fold_in(rng, 6), dim), (parts,), jnp.float32, smallest / len(cuts), high / len(cuts))
        return jnp.repeat(jnp.exp(steps), extent[dim] // parts).reshape((-1,) + (1,) * (len(extent) - dim - 1))

    loudness = one(*cuts[0])
    for cut in cuts[1:]:
        loudness = loudness * one(*cut)
    return loudness


def noise(key, dims, scale, reach, cuts=(), kind=jnp.bfloat16):
    entries = jax.random.normal(key, dims, jnp.float32) * scale
    if len(cuts) > 0:
        entries = block_scale(key, dims, cuts, -0.22, 0.18) * entries
    return jnp.clip(entries, min=-reach, max=reach).astype(kind)


def setup_inputs(seed: int = 0, part: int = 0) -> dict:
    streams_of = jax.random.split(jax.random.key(seed), 8)
    part_splits = jax.random.split(jax.random.fold_in(streams_of[7], part), 8)
    tokens = noise(part_splits[0], (TOKENS, D), 1.0, 6.0, ((0, 4),))
    neighbor_bank = draw_neighbor_bank(jax.random.fold_in(jax.random.fold_in(streams_of[7], part), 71), part)
    slots = plant(jax.random.randint(part_splits[2], (BLOCKS,), 0, BLOCK_DEV), jax.random.fold_in(part_splits[2], 1), 0, BLOCK_DEV - 1).astype(jnp.int32)
    w_query = noise(streams_of[3], (D, D), D ** -0.5, 0.125, ((0, 4), (1, 4)))
    w_key = noise(streams_of[4], (D, D), D ** -0.5, 0.125, ((0, 4), (1, 4)))
    w_value = noise(streams_of[5], (D, D), D ** -0.5, 0.125, ((0, 4), (1, 4)))
    w_out = noise(streams_of[6], (D, D), D ** -0.5, 0.125, ((0, 4), (1, 4)))
    return {"tokens": tokens, "neighbor_bank": neighbor_bank, "slots": slots, "w_query": w_query, "w_key": w_key, "w_value": w_value, "w_out": w_out}


def rms_normed(tokens):
    hidden = tokens.astype(jnp.float32)
    scale_row = lax.rsqrt(lax.optimization_barrier(jnp.mean(hidden * hidden, axis=-1, keepdims=True)) + 1e-06)
    return (hidden * scale_row).astype(jnp.bfloat16)

def reference(tokens, neighbor_bank, slots, w_query, w_key, w_value, w_out):
    normed = rms_normed(tokens)
    queries = jnp.dot(normed, w_query, preferred_element_type=jnp.float32).astype(jnp.bfloat16)
    block_ids = jnp.arange(BLOCKS, dtype=jnp.int32)
    bank_rows = (block_ids // BLOCK_DEV * BLOCK_DEV + slots).astype(jnp.int32)
    retrieved = jnp.take(neighbor_bank, bank_rows, axis=0).reshape(BLOCKS * NEIGHBORS * NEIGH_LEN, D)
    key_rows = jnp.dot(retrieved, w_key, preferred_element_type=jnp.float32).astype(jnp.bfloat16)
    value_rows = jnp.dot(retrieved, w_value, preferred_element_type=jnp.float32).astype(jnp.bfloat16)
    key_rows = key_rows.reshape(BLOCKS, NEIGHBORS * NEIGH_LEN, HEADS, HEAD_DIM)
    value_rows = value_rows.reshape(BLOCKS, NEIGHBORS * NEIGH_LEN, HEADS, HEAD_DIM)
    padding = jnp.zeros((1, NEIGHBORS * NEIGH_LEN, HEADS, HEAD_DIM), jnp.bfloat16)
    prior_keys = jnp.concatenate([padding, key_rows[:-1]], axis=0)
    prior_values = jnp.concatenate([padding, value_rows[:-1]], axis=0)
    query_blocks = queries.reshape(BLOCKS, BLOCK, HEADS, HEAD_DIM)
    scores = jnp.einsum('cmhd,cnhd->chmn', query_blocks.astype(jnp.float32), prior_keys.astype(jnp.float32)) / math.sqrt(HEAD_DIM)
    peak_score = lax.optimization_barrier(jnp.max(scores, axis=-1, keepdims=True))
    exponent = jnp.exp(scores - peak_score)
    weights = (exponent / lax.optimization_barrier(jnp.sum(exponent, axis=-1, keepdims=True))).astype(jnp.bfloat16)
    attended = jnp.einsum('chmn,cnhd->cmhd', weights.astype(jnp.float32), prior_values.astype(jnp.float32))
    attended = attended.astype(jnp.bfloat16).reshape(TOKENS, D)
    return jnp.dot(attended, w_out, preferred_element_type=jnp.float32).astype(jnp.bfloat16)
```

```python
import functools
import math

import jax
import jax.numpy as jnp
from jax import lax
from jax.experimental import pallas as pl
from jax.experimental.pallas import tpu as pltpu
from jax.sharding import PartitionSpec as P

HEAD_DIM = 128
F32 = jnp.float32
BF16 = jnp.bfloat16


COMM = True
COMP = True


def fused(S, H, NS, per, tokens, bank, slots, w_query, w_key, w_value, w_out, out,
          G, WO, tok, normed, rows_in, halo_out, halo_in, qb, att, acc,
          ld_sem, wl_sem, zr, xr, send_r, send_l, send_x,
          wzr, wxr, wsend_r, wsend_l, wsend_x, turn_s, turn_r, turn_l,
          hz_s, hz_r, hd_s, hd_r, att_s, att_r):
    s, h, b = lax.axis_index("seq"), lax.axis_index("head"), lax.axis_index("batch")
    nblk, nrow, D = bank.shape
    T = tokens.shape[0]
    blk = T // nblk
    CW = HEAD_DIM
    RS = w_query.shape[0]
    RH = RS // 2
    KO = H * CW
    KH = KO // 2
    KQ = KH // 2
    NW = 2 * NS
    groups = nblk // per
    GR = per * blk
    HR = nrow // 2

    def dev(seq, head, batch):
        return {"seq": seq, "head": head, "batch": batch}

    def rcopy(src, dst, ss, rs, device):
        return pltpu.make_async_remote_copy(
            src_ref=src, dst_ref=dst, send_sem=ss, recv_sem=rs,
            device_id=device, device_id_type=pl.DeviceIdType.MESH)

    w_loads = []
    for j in range(NS):
        for k, w in enumerate((w_query, w_key, w_value)):
            c = pltpu.make_async_copy(
                w.at[:, pl.ds(j * CW, CW)],
                G.at[j, pl.ds(s * RS, RS), pl.ds(k * CW, CW)], wl_sem.at[k * NS + j])
            c.start()
            w_loads.append(c)
    wo_own = pltpu.make_async_copy(w_out, WO.at[:, pl.ds(h * CW, CW), :], turn_l)

    @pl.when(h == s)
    def _():
        wo_own.start()
    tok_load = pltpu.make_async_copy(tokens, tok, ld_sem.at[nblk])
    tok_load.start()
    bank_loads = [pltpu.make_async_copy(bank.at[i], rows_in.at[i], ld_sem.at[i]) for i in range(nblk)]
    for c in bank_loads:
        c.start()

    barrier = pltpu.get_barrier_semaphore()
    for i in range(S):
        for k in range(H):
            @pl.when(jnp.logical_or(s != i, h != k))
            def _():
                pl.semaphore_signal(barrier, inc=1, device_id=dev(i, k, b), device_id_type=pl.DeviceIdType.MESH)
    pl.semaphore_signal(barrier, inc=1, device_id=dev(s, h, 1 - b), device_id_type=pl.DeviceIdType.MESH)
    pl.semaphore_wait(barrier, S * H)

    def chunk(t, origin, half):
        return G.at[t, pl.ds(origin * RS + half * RH, RH), :]

    edge = jnp.logical_or(s == 0, s == S - 1)
    middle = jnp.logical_and(s > 0, s < S - 1)
    near_dev = (s - 1) * 3
    far_dev = 3 - s
    edge_dev = 1 + s // 3

    def near(t, origin):
        return rcopy(chunk(t, origin, b), chunk(t, origin, b), send_r.at[t, origin], zr.at[t, origin],
                     dev(near_dev, h, b))

    def far(t, origin):
        return rcopy(chunk(t, origin, b), chunk(t, origin, b), send_l.at[t, origin], zr.at[t, origin],
                     dev(far_dev, h, b))

    def inward(t):
        return rcopy(chunk(t, s, b), chunk(t, s, b), send_r.at[t, s], zr.at[t, s], dev(edge_dev, h, b))

    def twin(t, origin, half):
        return rcopy(chunk(t, origin, half), chunk(t, origin, half), send_x.at[t, origin], xr.at[t, origin],
                     dev(s, h, 1 - b))

    def edge_event(t, d):
        o = d + (s // 3) * (3 - 2 * d)
        inward_from(t, o).wait_recv()
        twin(t, o, b).start()

    def inward_from(t, o):
        return rcopy(chunk(t, o, b), chunk(t, o, b), send_r.at[t, o], zr.at[t, o], dev(edge_dev, h, b))

    def mid_first(t):
        a, e = 3 - s, 3 * (s - 1)
        far(t, a).wait_recv()
        near(t, a).start()
        twin(t, a, b).start()
        far(t, e).wait_recv()
        far(t, e).start()
        twin(t, e, b).start()

    def mid_second(t):
        o = 3 * (2 - s)
        near(t, o).wait_recv()
        near(t, o).start()
        twin(t, o, b).start()

    def turn(j, device):
        return rcopy(w_out, WO.at[:, pl.ds(j * CW, CW), :], turn_s, turn_r.at[j], device)

    def wpart(k, half):
        return WO.at[k // 2, pl.ds(half * KH + (k % 2) * KQ, KQ), :]

    def wright(k):
        return rcopy(wpart(k, b), wpart(k, b), wsend_r.at[k], wzr.at[k], dev(lax.rem(s + 1, S), h, b))

    def wleft(k):
        return rcopy(wpart(k, b), wpart(k, b), wsend_l.at[k], wzr.at[k], dev(lax.rem(s + S - 1, S), h, b))

    def wtwin(k, half):
        return rcopy(wpart(k, half), wpart(k, half), wsend_x.at[k], wxr.at[k], dev(s, h, 1 - b))

    def wo_turned():
        wo_own.wait()
        for j in range(H):
            @pl.when(j != h)
            def _():
                turn(j, dev(s, s, b)).wait_recv()

    def wo_out(rightward):
        for k in range(NW):
            @pl.when(jnp.logical_and(rightward, s < S - 1))
            def _():
                wright(k).start()

            @pl.when(jnp.logical_and(jnp.logical_not(rightward), s > 0))
            def _():
                wleft(k).start()

    def wrelay(k):
        wright(k).wait_recv()

        @pl.when(jnp.logical_and(s > h, s < S - 1))
        def _():
            wright(k).start()

        @pl.when(jnp.logical_and(s < h, s > 0))
        def _():
            wleft(k).start()
        wtwin(k, b).start()

    side = lax.rem(h, 2)
    lead = h >= H // 2
    mate = (h // 2) * 2 + 1 - side
    peers = (mate, lax.rem(h + 2, H), lax.rem(mate + 2, H))

    def halo_z():
        return rcopy(halo_out, halo_in.at[pl.ds(side * HR, HR)], hz_s, hz_r, dev(lax.rem(s + 1, S), h, b))

    def halo_across():
        part = halo_in.at[pl.ds(side * HR, HR)]
        return rcopy(part, part, hd_s.at[0], hd_r.at[0], dev(s, lax.rem(h + 2, H), b))

    def halo_mate(half):
        part = halo_in.at[pl.ds(half * HR, HR)]
        return rcopy(part, part, hd_s.at[1], hd_r.at[1], dev(s, mate, b))

    def halo_spread():
        @pl.when(jnp.logical_and(lead, s > 0))
        def _():
            halo_z().wait_recv()
            halo_across().start()
            halo_mate(side).start()

    def halo_pass():
        @pl.when(jnp.logical_and(jnp.logical_not(lead), s > 0))
        def _():
            halo_across().wait_recv()
            halo_mate(side).start()

    def halo_take():
        @pl.when(s > 0)
        def _():
            halo_mate(1 - side).wait_recv()
            rows_in[nblk] = halo_in[...]

    def att_send(t, g, k):
        part = att.at[t, h, pl.ds(g * GR, GR), :]
        return rcopy(part, part, att_s.at[t, g, k], att_r.at[t, g, k], dev(s, peers[k], b))

    def att_wait(t, g, k):
        part = att.at[t, peers[k], pl.ds(g * GR, GR), :]
        return rcopy(part, part, att_s.at[t, g, k], att_r.at[t, g, k], dev(s, peers[k], b))

    scale = math.log2(math.e) / math.sqrt(HEAD_DIM)

    def unit(t, g):
        if COMP:
            rows = []
            for i in range(per):
                c = g * per + i
                at = slots[jnp.maximum(c - 1, 0)]
                rows.append(rows_in[jnp.where(c == 0, nblk, at)])
            kv = jnp.dot(jnp.concatenate(rows, axis=0), G[t, :, pl.ds(CW, 2 * CW)],
                         preferred_element_type=F32).astype(BF16)
            scores = []
            for i in range(per):
                q = qb[lax.rem(t, 2), pl.ds((g * per + i) * blk, blk), :]
                scores.append(lax.dot_general(q, kv[i * nrow:(i + 1) * nrow, :CW], (((1,), (1,)), ((), ())),
                                              preferred_element_type=F32))
            for i in range(per):
                e = jnp.exp2((scores[i] - jnp.max(scores[i], axis=-1, keepdims=True)) * scale)
                p = (e * (1.0 / jnp.sum(e, axis=-1, keepdims=True))).astype(BF16)
                o = jnp.dot(p, kv[i * nrow:(i + 1) * nrow, CW:], preferred_element_type=F32)
                att[t, h, pl.ds((g * per + i) * blk, blk), :] = o.astype(BF16)
        if COMM:
            for k in range(3):
                att_send(t, g, k).start()

    def queries(t):
        if COMP:
            qb[lax.rem(t, 2)] = jnp.dot(normed[...], G[t, :, pl.ds(0, CW)], preferred_element_type=F32).astype(BF16)

    def loaded(j):
        for c in w_loads[3 * j:3 * j + 3]:
            c.wait()

    loaded(0)
    if COMM:
        @pl.when(middle)
        def _():
            near(0, s).start()
            far(0, s).start()

        @pl.when(edge)
        def _():
            inward(0).start()
    loaded(1)
    if COMM:
        @pl.when(middle)
        def _():
            near(1, s).start()

        @pl.when(edge)
        def _():
            inward(1).start()

        @pl.when(h != s)
        def _():
            turn(h, dev(s, s, b)).start()
    loaded(2)
    loaded(3)
    if COMM:
        @pl.when(edge)
        def _():
            inward(2).start()
            inward(3).start()

    @pl.when(s == 0)
    def _():
        rows_in[nblk] = jnp.zeros((nrow, D), BF16)

    for c in bank_loads:
        c.wait()
    if COMM:
        @pl.when(jnp.logical_and(lead, s < S - 1))
        def _():
            halo_out[...] = rows_in[slots[nblk - 1], pl.ds(side * HR, HR), :]
            halo_z().start()

    tok_load.wait()

    def norm(i, _):
        x = tok[pl.ds(i * blk, blk), :].astype(F32)
        normed[pl.ds(i * blk, blk), :] = (
            x * lax.rsqrt(jnp.mean(x * x, axis=-1, keepdims=True) + 1e-06)).astype(BF16)
        return 0
    if COMP:
        lax.fori_loop(0, nblk, norm, 0)

    def first_edge():
        for t, d in ((0, 1), (1, 1), (0, 2), (0, 3), (2, 1)):
            edge_event(t, d)

        @pl.when(h == s)
        def _():
            wo_turned()
            wo_out(s == 0)

    def first_mid():
        mid_first(0)
        far(1, s).start()
        mid_second(0)
        near(2, s).start()
        mid_first(1)
        far(2, s).start()
        mid_second(1)
        near(3, s).start()

    edge_plan = {0: ((1, 2),), 1: ((1, 3),), 3: ((3, 1),), 4: ((2, 2),), 5: ((2, 3),), 7: ((3, 2),), 8: ((3, 3),)}
    edge_w = {10: (0,), 11: (1,), 12: (2, 3), 13: (4,), 14: (5,), 15: (6,), 16: (7,)}
    early_w = {4: (0, 1), 5: (2, 3), 6: (4, 5), 7: (6, 7)}
    late_w = {7: (0, 1), 8: (2, 3), 9: (4,), 10: (5,), 11: (6,), 12: (7,)}

    def events(n):
        @pl.when(edge)
        def _():
            for at, evs in edge_plan.items():
                @pl.when(n == at)
                def _():
                    for e in evs:
                        edge_event(*e)

            @pl.when(h != s)
            def _():
                for at, ks in edge_w.items():
                    @pl.when(n == at)
                    def _():
                        for k in ks:
                            wrelay(k)

        @pl.when(n == 0)
        def _():
            halo_spread()

        @pl.when(n == 5)
        def _():
            halo_pass()

        @pl.when(middle)
        def _():
            @pl.when(n == 0)
            def _():
                mid_first(2)
                far(3, s).start()

            @pl.when(n == 1)
            def _():
                mid_second(2)

            @pl.when(n == 3)
            def _():
                mid_first(3)

                @pl.when(h == s)
                def _():
                    wo_turned()
                    wo_out(s == 1)

            @pl.when(n == 4)
            def _():
                mid_second(3)

                @pl.when(h == s)
                def _():
                    wo_out(s == 2)

            @pl.when(h == near_dev)
            def _():
                for at, ks in early_w.items():
                    @pl.when(n == at)
                    def _():
                        for k in ks:
                            wrelay(k)

            @pl.when(jnp.logical_and(h != near_dev, h != s))
            def _():
                for at, ks in late_w.items():
                    @pl.when(n == at)
                    def _():
                        for k in ks:
                            wrelay(k)

    if COMM:
        @pl.when(edge)
        def _():
            first_edge()

        @pl.when(middle)
        def _():
            first_mid()

    def slot(n, _):
        t, gi = n // groups, lax.rem(n, groups)

        @pl.when(jnp.logical_and(gi == 0, t < NS))
        def _():
            if COMM:
                for o in range(S):
                    @pl.when(s != o)
                    def _():
                        twin(t, o, 1 - b).wait_recv()
            queries(t)

        @pl.when(n == 2 * groups - 1)
        def _():
            if COMM:
                halo_take()
        last = jnp.logical_or(gi == groups - 1, t == NS)
        u = jnp.where(last, t - 1, t)

        @pl.when(u >= 0)
        def _():
            unit(u, jnp.where(last, 0, gi + 1))
        if COMM:
            events(n)
        return 0

    lax.fori_loop(0, NS * groups + 1, slot, 0)

    tile = T // 4

    def fold(j, _):
        if COMM:
            @pl.when(h != s)
            def _():
                for k in range(2):
                    wtwin(2 * j + k, 1 - b).wait_recv()

            def arrived(g, _):
                for k in range(3):
                    att_wait(j, g, k).wait_recv()
                return 0
            lax.fori_loop(0, groups, arrived, 0)

        def rows(i, _):
            r = pl.ds(i * tile, tile)
            part = jnp.dot(jnp.concatenate([att[j, k, r, :] for k in range(H)], axis=1), WO[j],
                           preferred_element_type=F32)

            @pl.when(j == 0)
            def _():
                acc[r, :] = part

            @pl.when(jnp.logical_and(j > 0, j < NS - 1))
            def _():
                acc[r, :] += part

            @pl.when(j == NS - 1)
            def _():
                out[r, :] = (acc[r, :] + part).astype(BF16)
            return 0
        if COMP:
            lax.fori_loop(0, 4, rows, 0)
        return 0
    lax.fori_loop(0, NS, fold, 0)

    def drain(t, _):
        @pl.when(edge)
        def _():
            inward(t).wait_send()

        @pl.when(middle)
        def _():
            for o in (s, 3 - s, 3 * (2 - s)):
                near(t, o).wait_send()
            for o in (s, 3 * (s - 1)):
                far(t, o).wait_send()
        for o in range(S):
            @pl.when(s != o)
            def _():
                twin(t, o, b).wait_send()

        def sent(g, _):
            for k in range(3):
                att_send(t, g, k).wait_send()
            return 0
        lax.fori_loop(0, groups, sent, 0)

        for k in (2 * t, 2 * t + 1):
            @pl.when(jnp.logical_and(s >= h, s < S - 1))
            def _():
                wright(k).wait_send()

            @pl.when(jnp.logical_and(s <= h, s > 0))
            def _():
                wleft(k).wait_send()

            @pl.when(h != s)
            def _():
                wtwin(k, b).wait_send()
        return 0
    if COMM:
        lax.fori_loop(0, NS, drain, 0)

        @pl.when(h != s)
        def _():
            turn(h, dev(s, s, b)).wait_send()

        @pl.when(jnp.logical_and(lead, s < S - 1))
        def _():
            halo_z().wait_send()

        @pl.when(s > 0)
        def _():
            halo_mate(side).wait_send()

            @pl.when(lead)
            def _():
                halo_across().wait_send()
    else:
        @pl.when(h == s)
        def _():
            wo_own.wait()


def one_kernel(tokens, neighbor_bank, slots, w_query, w_key, w_value, w_out):
    S, H = lax.axis_size("seq"), lax.axis_size("head")
    T, D = tokens.shape
    nblk, nrow = neighbor_bank.shape[:2]
    width = w_query.shape[1]
    NS = width // HEAD_DIM
    CW = HEAD_DIM
    out_cols = D // H
    per = nblk // 4
    groups = nblk // per
    dma = pltpu.SemaphoreType.DMA
    hbm = pl.BlockSpec(memory_space=pl.ANY)
    return pl.pallas_call(
        functools.partial(fused, S, H, NS, per),
        out_shape=jax.ShapeDtypeStruct((T, out_cols), BF16),
        in_specs=[hbm, hbm, pl.BlockSpec(memory_space=pltpu.SMEM), hbm, hbm, hbm, hbm],
        out_specs=pl.BlockSpec(memory_space=pltpu.VMEM),
        scratch_shapes=[
            pltpu.VMEM((NS, D, 3 * CW), BF16),
            pltpu.VMEM((NS, H * CW, out_cols), BF16),
            pltpu.VMEM((T, D), BF16),
            pltpu.VMEM((T, D), BF16),
            pltpu.VMEM((nblk + 1, nrow, D), BF16),
            pltpu.VMEM((nrow // 2, D), BF16),
            pltpu.VMEM((nrow, D), BF16),
            pltpu.VMEM((2, T, CW), BF16),
            pltpu.VMEM((NS, H, T, CW), BF16),
            pltpu.VMEM((T, out_cols), F32),
            dma((nblk + 1,)),
            dma((3 * NS,)),
            dma((NS, S)), dma((NS, S)), dma((NS, S)), dma((NS, S)), dma((NS, S)),
            dma((2 * NS,)), dma((2 * NS,)), dma((2 * NS,)), dma((2 * NS,)), dma((2 * NS,)), dma, dma((H,)), dma,
            dma, dma, dma((2,)), dma((2,)),
            dma((NS, groups, 3)), dma((NS, groups, 3)),
        ],
        compiler_params=pltpu.CompilerParams(
            collective_id=0, has_side_effects=True, vmem_limit_bytes=63 * 1024 * 1024),
    )(tokens, neighbor_bank, slots, w_query, w_key, w_value, w_out.reshape(NS, CW, -1))


def passed_along(block, axis, distance):
    devices = range(lax.axis_size(axis))
    route = [(i - distance, i) for i in devices if i - distance in devices]
    return lax.ppermute(block, axis, route)


def attend(query_blocks, key_blocks, value_blocks):
    scores = jnp.einsum(
        "cmhd,cnhd->chmn", query_blocks, key_blocks, preferred_element_type=jnp.float32
    ) / math.sqrt(HEAD_DIM)
    peak_score = jnp.max(scores, axis=-1, keepdims=True)
    exponent = jnp.exp(scores - peak_score)
    weights = (exponent / jnp.sum(exponent, axis=-1, keepdims=True)).astype(jnp.bfloat16)
    blended = jnp.einsum(
        "chmn,cnhd->cmhd", weights, value_blocks, preferred_element_type=jnp.float32
    ).astype(jnp.bfloat16)
    return blended.reshape(blended.shape[0] * blended.shape[1], blended.shape[2] * blended.shape[3])


def fold_rows(source, shard_rows):
    return jnp.dot(source, shard_rows, preferred_element_type=jnp.float32)


def local(tokens, neighbor_bank, slots, w_query, w_key, w_value, w_out):
    tok_rows, model_width = tokens.shape
    block_count = neighbor_bank.shape[0]
    neighbor_rows = neighbor_bank.shape[1]
    block_len = tok_rows // block_count
    local_width = w_query.shape[1]
    local_heads = local_width // HEAD_DIM
    hidden = tokens.astype(jnp.float32)
    normed = (hidden * lax.rsqrt(jnp.mean(hidden * hidden, axis=-1, keepdims=True) + 1e-06)).astype(
        jnp.bfloat16
    )
    retrieved = jnp.take(neighbor_bank, slots, axis=0)
    arrived = passed_along(retrieved[block_count - 1], "seq", 1)
    context = jnp.concatenate([arrived[None], retrieved[: block_count - 1]], axis=0)
    context_flat = context.reshape(block_count * neighbor_rows, model_width)
    query_sum = fold_rows(normed, lax.all_gather(w_query, "seq", axis=0, tiled=True))
    key_sum = fold_rows(context_flat, lax.all_gather(w_key, "seq", axis=0, tiled=True))
    value_sum = fold_rows(context_flat, lax.all_gather(w_value, "seq", axis=0, tiled=True))
    query_blocks = query_sum.astype(jnp.bfloat16).reshape(
        block_count, block_len, local_heads, HEAD_DIM
    )
    key_blocks = key_sum.astype(jnp.bfloat16).reshape(
        block_count, neighbor_rows, local_heads, HEAD_DIM
    )
    value_blocks = value_sum.astype(jnp.bfloat16).reshape(
        block_count, neighbor_rows, local_heads, HEAD_DIM
    )
    attended = attend(query_blocks, key_blocks, value_blocks)
    every_head = lax.all_gather(attended, "head", axis=1, tiled=True)
    wide_rows = lax.all_gather(w_out, "seq", axis=1, tiled=True)
    own_columns = lax.all_to_all(wide_rows, "head", split_axis=1, concat_axis=0, tiled=True)
    return jnp.dot(every_head, own_columns, preferred_element_type=jnp.float32).astype(jnp.bfloat16)


def solution(mesh):
    in_specs = (
        P(("batch", "seq"), None),
        P(("batch", "seq"), None, None),
        P(("batch", "seq")),
        P("seq", "head"),
        P("seq", "head"),
        P("seq", "head"),
        P("head", "seq"),
    )
    out_specs = P(("batch", "seq"), "head")
    square = mesh.shape["seq"] == 4 and mesh.shape["head"] == 4 and mesh.shape["batch"] == 2
    body = one_kernel if square else local
    return jax.shard_map(body, mesh=mesh, in_specs=in_specs, out_specs=out_specs, check_vma=False)
```

```python
import functools
import math

import jax
import jax.numpy as jnp
from jax import lax
from jax.experimental import pallas as pl
from jax.experimental.pallas import tpu as pltpu
from jax.sharding import PartitionSpec as P

HEAD_DIM = 128
F32 = jnp.float32
BF16 = jnp.bfloat16


NZ, NX = 9, 7
HALO_FIRST = 2
EDGE_QKV = {0: ((1, 2),), 1: ((1, 3),), 2: ((2, 2),), 3: ((2, 3),), 4: ((3, 1),), 5: ((3, 2),), 6: ((3, 3),)}
EDGE_W = {7: (0,), 8: (1,), 9: (2,), 10: (3,), 11: (4,)}
EDGE_W_LATE = {9: (0, 1), 10: (2,), 11: (3, 4)}
EDGE_W_TAIL = ((5,), (), (6,), (7, 8))
VMEM_MIB = 48
MID_W_EARLY = {2: (0, 1), 3: (2, 3), 4: (4, 5), 5: (6, 7, 8)}
MID_W = {5: (0, 1), 6: (2, 3, 4), 7: (5,), 8: (6,), 9: (7, 8)}
HALO_SPREAD = {5: (0, 1), 8: (2, 3)}
HALO_PASS = {8: (0,), 9: (1,), 12: (2, 3)}
COMM = True
COMP = True


def fused(S, H, NS, tokens, bank, slots, w_query, w_key, w_value, w_out, out,
          G, WO, tok, normed, rows_in, halo_out, halo_in, qb, att, acc,
          ld_sem, wl_sem, zr, xr, send_n, send_f, send_x,
          wzr, wxr, wsend_r, wsend_l, wsend_x, turn_s, turn_r, turn_l,
          hz_s, hz_r, hy_s, hy_r, hm_s, hm_r, att_s, att_y, att_m, att_b):
    s, h, b = lax.axis_index("seq"), lax.axis_index("head"), lax.axis_index("batch")
    nblk, nrow, D = bank.shape
    T = tokens.shape[0]
    blk = T // nblk
    CW = HEAD_DIM
    RS = w_query.shape[0]
    RH = RS // 2
    KH = H * CW // 2
    KQ = KH // 2
    NW = 2 * NS
    units = 3
    per = (nblk - 1) // units
    GR = per * blk
    HR = nrow // 2
    HP = HR // NS

    def dev(seq, head, batch):
        return {"seq": seq, "head": head, "batch": batch}

    def rcopy(src, dst, ss, rs, device):
        return pltpu.make_async_remote_copy(
            src_ref=src, dst_ref=dst, send_sem=ss, recv_sem=rs,
            device_id=device, device_id_type=pl.DeviceIdType.MESH)

    edge = jnp.logical_or(s == 0, s == S - 1)
    middle = jnp.logical_and(s > 0, s < S - 1)
    near_dev = (s - 1) * 3
    far_dev = 3 - s
    edge_dev = 1 + s // 3
    side = lax.rem(h, 2)
    lead = h >= H // 2
    mate = (h // 2) * 2 + 1 - side
    across = lax.rem(h + 2, H)
    peers = (mate, across, lax.rem(mate + 2, H))

    w_loads = []
    for j in range(NS):
        for k, w in enumerate((w_query, w_key, w_value)):
            c = pltpu.make_async_copy(
                w.at[:, pl.ds(j * CW, CW)],
                G.at[j, pl.ds(s * RS, RS), pl.ds(k * CW, CW)], wl_sem.at[j])
            w_loads.append(c)
    for c in w_loads[:3]:
        c.start()
    wo_own = pltpu.make_async_copy(w_out, WO.at[:, pl.ds(h * CW, CW), :], turn_l)

    tok_load = pltpu.make_async_copy(tokens, tok, ld_sem.at[1])
    bank_loads = [pltpu.make_async_copy(bank.at[i], rows_in.at[i], ld_sem.at[0]) for i in range(nblk)]

    barrier = pltpu.get_barrier_semaphore()

    def greet(device):
        pl.semaphore_signal(barrier, inc=1, device_id=device, device_id_type=pl.DeviceIdType.MESH)

    for p in peers:
        greet(dev(s, p, b))
    greet(dev(s, h, 1 - b))

    @pl.when(edge)
    def _():
        greet(dev(edge_dev, h, b))
        pl.semaphore_wait(barrier, 5)

    @pl.when(middle)
    def _():
        greet(dev(near_dev, h, b))
        greet(dev(far_dev, h, b))
        pl.semaphore_wait(barrier, 6)

    def chunk(t, origin, half):
        return G.at[t, pl.ds(origin * RS + half * RH, RH), :]

    def near(t, origin):
        return rcopy(chunk(t, origin, b), chunk(t, origin, b), send_n, zr.at[t, origin],
                     dev(near_dev, h, b))

    def far(t, origin):
        return rcopy(chunk(t, origin, b), chunk(t, origin, b), send_f, zr.at[t, origin],
                     dev(far_dev, h, b))

    def inward(t, origin):
        return rcopy(chunk(t, origin, b), chunk(t, origin, b), send_n, zr.at[t, origin],
                     dev(edge_dev, h, b))

    def twin(t, origin, half):
        return rcopy(chunk(t, origin, half), chunk(t, origin, half), send_x, xr.at[t],
                     dev(s, h, 1 - b))

    def edge_event(t, d):
        o = d + (s // 3) * (3 - 2 * d)
        inward(t, o).wait_recv()
        twin(t, o, b).start()

    def mid_first(t):
        a, e = 3 - s, 3 * (s - 1)

        def outer():
            far(t, e).wait_recv()
            far(t, e).start()
            twin(t, e, b).start()
        if t > 0:
            outer()
        far(t, a).wait_recv()
        near(t, a).start()
        twin(t, a, b).start()
        if t == 0:
            outer()

    def mid_second(t):
        o = 3 * (2 - s)
        near(t, o).wait_recv()
        near(t, o).start()
        twin(t, o, b).start()

    def turn(j, device):
        return rcopy(w_out, WO.at[:, pl.ds(j * CW, CW), :], turn_s, turn_r, device)

    def wpart(k, half):
        return WO.at[k // 2, pl.ds(half * KH + (k % 2) * KQ, KQ), :]

    def wpiece(k):
        return wpart(k, b) if k < NW else wpart(2 * NW - 1 - k, 1 - b)

    def wright(k):
        return rcopy(wpiece(k), wpiece(k), wsend_r, wzr.at[k], dev(lax.rem(s + 1, S), h, b))

    def wleft(k):
        return rcopy(wpiece(k), wpiece(k), wsend_l, wzr.at[k], dev(lax.rem(s + S - 1, S), h, b))

    def wtwin(k, half):
        return rcopy(wpart(k, half), wpart(k, half), wsend_x, wxr.at[k // (NX - 1)], dev(s, h, 1 - b))

    def wo_turned():
        wo_own.wait()
        three = WO.at[:, pl.ds(0, (H - 1) * CW), :]
        rcopy(three, three, turn_s, turn_r, dev(s, mate, b)).wait_recv()

    def wo_out(rightward):
        for k in range(NZ):
            @pl.when(jnp.logical_and(rightward, s < S - 1))
            def _():
                wright(k).start()

            @pl.when(jnp.logical_and(jnp.logical_not(rightward), s > 0))
            def _():
                wleft(k).start()

    def wrelay(k):
        wright(k).wait_recv()

        @pl.when(jnp.logical_and(s > h, s < S - 1))
        def _():
            wright(k).start()

        @pl.when(jnp.logical_and(s < h, s > 0))
        def _():
            wleft(k).start()
        if k < NX:
            wtwin(k, b).start()

    def halo_part(p, who):
        return halo_in.at[pl.ds(who * HR + p * HP, HP)]

    def halo_z(p):
        return rcopy(halo_out.at[pl.ds(p * HP, HP)], halo_part(p, side), hz_s, hz_r.at[p],
                     dev(lax.rem(s + 1, S), h, b))

    def halo_y(p):
        return rcopy(halo_part(p, side), halo_part(p, side), hy_s, hy_r.at[p], dev(s, across, b))

    def halo_m(p, who):
        return rcopy(halo_part(p, who), halo_part(p, who), hm_s, hm_r, dev(s, mate, b))

    def halo_spread(p):
        @pl.when(jnp.logical_and(lead, s > 0))
        def _():
            halo_z(p).wait_recv()
            halo_y(p).start()
            halo_m(p, side).start()

    def halo_pass(p):
        @pl.when(jnp.logical_and(jnp.logical_not(lead), s > 0))
        def _():
            halo_y(p).wait_recv()
            halo_m(p, side).start()

    def att_rows(t, who, g):
        if isinstance(g, int) and g == units:
            return att.at[t, who, pl.ds(0, blk), :]
        return att.at[t, who, pl.ds(blk + g * GR, GR), :]

    def att_copy(t, g, who, rs, device):
        return rcopy(att_rows(t, who, g), att_rows(t, who, g), att_s, rs, dev(s, device, b))

    def att_send(t, g):
        att_copy(t, g, h, att_m.at[0, t], mate).start()
        att_copy(t, g, h, att_y.at[t, g], across).start()

    def att_pass(t, g):
        att_copy(t, g, across, att_y.at[t, g], across).wait_recv()
        att_copy(t, g, across, att_m.at[1, t], mate).start()

    def att_got(t):
        for k in range(2):
            block = att.at[t, 0, pl.ds(blk, T - blk), :]
            rcopy(block, block, att_s, att_m.at[k, t], dev(s, mate, b)).wait_recv()

    def att_first(k, device):
        part = att.at[:, h, pl.ds(0, blk), :]
        return rcopy(part, part, att_s, att_b.at[k], dev(s, device, b))

    scale = math.log2(math.e) / math.sqrt(HEAD_DIM)

    def attend_all(blocks):
        scores = []
        for t, c, kv in blocks:
            q = qb[t, pl.ds(c * blk, blk), :]
            scores.append(lax.dot_general(q, kv[:, :CW], (((1,), (1,)), ((), ())), preferred_element_type=F32))
        for (t, c, kv), sc in zip(blocks, scores):
            e = jnp.exp2((sc - jnp.max(sc, axis=-1, keepdims=True)) * scale)
            p = (e * (1.0 / jnp.sum(e, axis=-1, keepdims=True))).astype(BF16)
            o = jnp.dot(p, kv[:, CW:], preferred_element_type=F32)
            att[t, h, pl.ds(c * blk, blk), :] = o.astype(BF16)

    def project(t, rows):
        return jnp.dot(rows, G[t, :, pl.ds(CW, 2 * CW)], preferred_element_type=F32).astype(BF16)

    def unit(t, g):
        first = 1 + g * per
        rows = [rows_in[slots[first + i - 1]] for i in range(per)]
        kv = project(t, jnp.concatenate(rows, axis=0))
        attend_all([(t, first + i, kv[i * nrow:(i + 1) * nrow]) for i in range(per)])

    def queries(t):
        qb[t] = jnp.dot(normed[...], G[t, :, pl.ds(0, CW)], preferred_element_type=F32).astype(BF16)

    def loaded(j):
        own = G.at[j, pl.ds(s * RS, RS), :]
        pltpu.make_async_copy(own, own, wl_sem.at[j]).wait()

    loaded(0)
    for c in w_loads[3:]:
        c.start()
    if COMM:
        @pl.when(middle)
        def _():
            near(0, s).start()
            far(0, s).start()

        @pl.when(edge)
        def _():
            inward(0, s).start()
    loaded(1)
    tok_load.start()

    @pl.when(h == s)
    def _():
        wo_own.start()
    for c in bank_loads:
        c.start()
    if COMM:
        @pl.when(middle)
        def _():
            near(1, s).start()

        @pl.when(edge)
        def _():
            inward(1, s).start()

        @pl.when(h != s)
        def _():
            turn(h, dev(s, s, b)).start()
    loaded(2)
    loaded(3)
    if COMM:
        @pl.when(edge)
        def _():
            inward(2, s).start()
            inward(3, s).start()

            edge_event(0, 1)

        @pl.when(middle)
        def _():
            mid_first(0)
            far(1, s).start()
    tok_load.wait()

    def norm(i, _):
        x = tok[pl.ds(i * blk, blk), :].astype(F32)
        normed[pl.ds(i * blk, blk), :] = (
            x * lax.rsqrt(jnp.mean(x * x, axis=-1, keepdims=True) + 1e-06)).astype(BF16)
        return 0
    if COMP:
        lax.fori_loop(0, nblk, norm, 0)

    pltpu.make_async_copy(bank, rows_in, ld_sem.at[0]).wait()
    if COMM:
        @pl.when(jnp.logical_and(lead, s < S - 1))
        def _():
            halo_out[...] = rows_in[slots[nblk - 1], pl.ds(side * HR, HR), :]

        @pl.when(s == 0)
        def _():
            halo_in[...] = jnp.zeros_like(halo_in)

        @pl.when(edge)
        def _():
            for t, d in ((1, 1), (0, 2), (0, 3), (2, 1)):
                edge_event(t, d)

            @pl.when(h == s)
            def _():
                wo_turned()
                wo_out(s == 0)

        @pl.when(middle)
        def _():
            mid_second(0)
            near(2, s).start()
            mid_first(1)
            far(2, s).start()
            mid_second(1)

    def halo_out_pieces(pieces):
        @pl.when(jnp.logical_and(lead, s < S - 1))
        def _():
            for p in pieces:
                halo_z(p).start()

    def plan(n, table, event):
        for at, items in table.items():
            @pl.when(n == at)
            def _():
                for item in items:
                    event(item)

    def events(n):
        @pl.when(edge)
        def _():
            plan(n, EDGE_QKV, lambda e: edge_event(*e))

            late = jnp.logical_and(s == S - 1, lead)

            @pl.when(jnp.logical_and(h != s, jnp.logical_not(late)))
            def _():
                plan(n, EDGE_W, wrelay)

            @pl.when(jnp.logical_and(h != s, late))
            def _():
                plan(n, EDGE_W_LATE, wrelay)

        @pl.when(middle)
        def _():
            @pl.when(n == 0)
            def _():
                mid_first(2)
                far(3, s).start()

            @pl.when(n == 1)
            def _():
                mid_second(2)

        @pl.when(n == 1)
        def _():
            halo_out_pieces(range(HALO_FIRST))

        @pl.when(middle)
        def _():
            @pl.when(n == 1)
            def _():
                near(3, s).start()

            @pl.when(n == 2)
            def _():
                mid_first(3)

                @pl.when(h == s)
                def _():
                    wo_turned()
                    wo_out(s == 1)

            @pl.when(n == 3)
            def _():
                mid_second(3)

        @pl.when(n == 3)
        def _():
            halo_out_pieces(range(HALO_FIRST, NS))

            @pl.when(jnp.logical_and(middle, h == s))
            def _():
                wo_out(s == 2)

        @pl.when(middle)
        def _():
            @pl.when(h == near_dev)
            def _():
                plan(n, MID_W_EARLY, wrelay)

            @pl.when(jnp.logical_and(h != near_dev, h != s))
            def _():
                plan(n, MID_W, wrelay)
        plan(n, HALO_SPREAD, halo_spread)
        plan(n, HALO_PASS, halo_pass)

    def slot(n, _):
        t, g = n // units, lax.rem(n, units)

        @pl.when(g == 0)
        def _():
            if COMM:
                twin_span = G.at[t, pl.ds(0, (S - 1) * RH), :]
                rcopy(twin_span, twin_span, send_x, xr.at[t], dev(s, h, 1 - b)).wait_recv()
            if COMP:
                queries(t)
        if COMP:
            unit(t, g)
        if COMM:
            att_send(t, g)
            events(n)

            @pl.when(t > 0)
            def _():
                att_pass(t - 1, g)
        return 0

    lax.fori_loop(0, NS * units, slot, 0)

    def edge_w(ks):
        @pl.when(jnp.logical_and(edge, h != s))
        def _():
            for k in ks:
                wrelay(k)

    def wrows(n):
        return WO.at[:, pl.ds(0, n * KQ // NS), :]

    def wx_got(i, n):
        @pl.when(h != s)
        def _():
            rcopy(wrows(n), wrows(n), wsend_x, wxr.at[i], dev(s, h, 1 - b)).wait_recv()

    def gathered(ts, rows):
        return jnp.concatenate([att[t, k, rows, :] for t in ts for k in range(H)], axis=1)

    early = range(NS - 1)

    def fold_early(g, _):
        r = pl.ds(blk + g * GR, GR)
        acc[r, :] = jnp.dot(gathered(early, r), WO[0:NS - 1].reshape((NS - 1) * H * CW, -1),
                            preferred_element_type=F32)
        return 0

    if COMM:
        edge_w(EDGE_W_TAIL[0])
        plan(NS * units, HALO_PASS, halo_pass)
        edge_w(EDGE_W_TAIL[1])

        @pl.when(s > 0)
        def _():
            half = halo_in.at[pl.ds(0, HR)]
            rcopy(half, half, hm_s, hm_r, dev(s, mate, b)).wait_recv()
    if COMP:
        attend_all([(t, 0, project(t, halo_in[...])) for t in range(NS)])
    if COMM:
        for k in range(3):
            att_first(k, peers[k]).start()
        edge_w(EDGE_W_TAIL[2])
        for g in range(units):
            att_pass(NS - 1, g)
        for t in early:
            att_got(t)
        wx_got(0, NX - 1)
    if COMP:
        lax.fori_loop(0, units, fold_early, 0)
    if COMM:
        edge_w(EDGE_W_TAIL[3])
        wx_got(1, 1)
        att_got(NS - 1)

    def fold_late(g, _):
        r = pl.ds(blk + g * GR, GR)
        if COMP:
            part = jnp.dot(gathered((NS - 1,), r), WO[NS - 1], preferred_element_type=F32)
            out[r, :] = (acc[r, :] + part).astype(BF16)
        return 0
    lax.fori_loop(0, units, fold_late, 0)
    if COMM:
        for k in range(3):
            att_first(k, peers[k]).wait_recv()
    first = pl.ds(0, blk)
    if COMP:
        out[first, :] = jnp.dot(gathered(range(NS), first), WO[...].reshape(NS * H * CW, -1),
                                preferred_element_type=F32).astype(BF16)

    def drained(span, sem, device):
        rcopy(span, span, sem, hm_r, device).wait_send()

    if COMM:
        beside = dev(s, mate, b)

        @pl.when(edge)
        def _():
            drained(G.at[:, pl.ds(0, RH), :], send_n, beside)

        @pl.when(middle)
        def _():
            drained(G.at[:, pl.ds(0, 3 * RH), :], send_n, beside)
            drained(G.at[:, pl.ds(0, 2 * RH), :], send_f, beside)
        drained(G.at[:, pl.ds(0, (S - 1) * RH), :], send_x, beside)
        drained(att.at[:, 0:3], att_s, beside)

        @pl.when(jnp.logical_and(lead, s < S - 1))
        def _():
            drained(halo_out, hz_s, beside)

        @pl.when(s > 0)
        def _():
            drained(halo_in.at[pl.ds(0, HR)], hm_s, beside)

            @pl.when(lead)
            def _():
                drained(halo_in.at[pl.ds(0, HR)], hy_s, beside)

        @pl.when(jnp.logical_and(s >= h, s < S - 1))
        def _():
            drained(wrows(NZ), wsend_r, beside)

        @pl.when(jnp.logical_and(s <= h, s > 0))
        def _():
            drained(wrows(NZ), wsend_l, beside)

        @pl.when(h != s)
        def _():
            drained(wrows(NX), wsend_x, beside)
            drained(w_out, turn_s, beside)
    else:
        @pl.when(h == s)
        def _():
            wo_own.wait()


def one_kernel(tokens, neighbor_bank, slots, w_query, w_key, w_value, w_out):
    S, H = lax.axis_size("seq"), lax.axis_size("head")
    T, D = tokens.shape
    nblk, nrow = neighbor_bank.shape[:2]
    width = w_query.shape[1]
    NS = width // HEAD_DIM
    CW = HEAD_DIM
    out_cols = D // H
    dma = pltpu.SemaphoreType.DMA
    hbm = pl.BlockSpec(memory_space=pltpu.HBM)
    tokens, neighbor_bank, slots, w_query, w_key, w_value, w_out = [
        pltpu.with_memory_space_constraint(x, pltpu.HBM)
        for x in (tokens, neighbor_bank, slots, w_query, w_key, w_value, w_out.reshape(NS, CW, -1))]
    return pl.pallas_call(
        functools.partial(fused, S, H, NS),
        out_shape=jax.ShapeDtypeStruct((T, out_cols), BF16),
        in_specs=[hbm, hbm, pl.BlockSpec(memory_space=pltpu.SMEM), hbm, hbm, hbm, hbm],
        out_specs=pl.BlockSpec(memory_space=pltpu.VMEM),
        scratch_shapes=[
            pltpu.VMEM((NS, D, 3 * CW), BF16),
            pltpu.VMEM((NS, H * CW, out_cols), BF16),
            pltpu.VMEM((T, D), BF16),
            pltpu.VMEM((T, D), BF16),
            pltpu.VMEM((nblk, nrow, D), BF16),
            pltpu.VMEM((nrow // 2, D), BF16),
            pltpu.VMEM((nrow, D), BF16),
            pltpu.VMEM((NS, T, CW), BF16),
            pltpu.VMEM((NS, H, T, CW), BF16),
            pltpu.VMEM((T, out_cols), F32),
            dma((2,)),
            dma((NS,)),
            dma((NS, S)), dma((NS,)), dma, dma, dma,
            dma((NZ,)), dma((2,)), dma, dma, dma, dma, dma, dma,
            dma, dma((NS,)), dma, dma((NS,)), dma, dma,
            dma, dma((NS, 3)), dma((2, NS)), dma((3,)),
        ],
        compiler_params=pltpu.CompilerParams(
            collective_id=0, has_side_effects=True, vmem_limit_bytes=VMEM_MIB * 1024 * 1024),
    )(tokens, neighbor_bank, slots, w_query, w_key, w_value, w_out)


def passed_along(block, axis, distance):
    devices = range(lax.axis_size(axis))
    route = [(i - distance, i) for i in devices if i - distance in devices]
    return lax.ppermute(block, axis, route)


def attend(query_blocks, key_blocks, value_blocks):
    scores = jnp.einsum(
        "cmhd,cnhd->chmn", query_blocks, key_blocks, preferred_element_type=jnp.float32
    ) / math.sqrt(HEAD_DIM)
    peak_score = jnp.max(scores, axis=-1, keepdims=True)
    exponent = jnp.exp(scores - peak_score)
    weights = (exponent / jnp.sum(exponent, axis=-1, keepdims=True)).astype(jnp.bfloat16)
    blended = jnp.einsum(
        "chmn,cnhd->cmhd", weights, value_blocks, preferred_element_type=jnp.float32
    ).astype(jnp.bfloat16)
    return blended.reshape(blended.shape[0] * blended.shape[1], blended.shape[2] * blended.shape[3])


def fold_rows(source, shard_rows):
    return jnp.dot(source, shard_rows, preferred_element_type=jnp.float32)


def local(tokens, neighbor_bank, slots, w_query, w_key, w_value, w_out):
    tok_rows, model_width = tokens.shape
    block_count = neighbor_bank.shape[0]
    neighbor_rows = neighbor_bank.shape[1]
    block_len = tok_rows // block_count
    local_width = w_query.shape[1]
    local_heads = local_width // HEAD_DIM
    hidden = tokens.astype(jnp.float32)
    normed = (hidden * lax.rsqrt(jnp.mean(hidden * hidden, axis=-1, keepdims=True) + 1e-06)).astype(
        jnp.bfloat16
    )
    retrieved = jnp.take(neighbor_bank, slots, axis=0)
    arrived = passed_along(retrieved[block_count - 1], "seq", 1)
    context = jnp.concatenate([arrived[None], retrieved[: block_count - 1]], axis=0)
    context_flat = context.reshape(block_count * neighbor_rows, model_width)
    query_sum = fold_rows(normed, lax.all_gather(w_query, "seq", axis=0, tiled=True))
    key_sum = fold_rows(context_flat, lax.all_gather(w_key, "seq", axis=0, tiled=True))
    value_sum = fold_rows(context_flat, lax.all_gather(w_value, "seq", axis=0, tiled=True))
    query_blocks = query_sum.astype(jnp.bfloat16).reshape(
        block_count, block_len, local_heads, HEAD_DIM
    )
    key_blocks = key_sum.astype(jnp.bfloat16).reshape(
        block_count, neighbor_rows, local_heads, HEAD_DIM
    )
    value_blocks = value_sum.astype(jnp.bfloat16).reshape(
        block_count, neighbor_rows, local_heads, HEAD_DIM
    )
    attended = attend(query_blocks, key_blocks, value_blocks)
    every_head = lax.all_gather(attended, "head", axis=1, tiled=True)
    wide_rows = lax.all_gather(w_out, "seq", axis=1, tiled=True)
    own_columns = lax.all_to_all(wide_rows, "head", split_axis=1, concat_axis=0, tiled=True)
    return jnp.dot(every_head, own_columns, preferred_element_type=jnp.float32).astype(jnp.bfloat16)


def solution(mesh):
    in_specs = (
        P(("batch", "seq"), None),
        P(("batch", "seq"), None, None),
        P(("batch", "seq")),
        P("seq", "head"),
        P("seq", "head"),
        P("seq", "head"),
        P("head", "seq"),
    )
    out_specs = P(("batch", "seq"), "head")
    square = mesh.shape["seq"] == 4 and mesh.shape["head"] == 4 and mesh.shape["batch"] == 2
    body = one_kernel if square else local
    return jax.shard_map(body, mesh=mesh, in_specs=in_specs, out_specs=out_specs, check_vma=False)
```

```python
import functools
import math

import jax
import jax.numpy as jnp
from jax import lax
from jax.experimental import pallas as pl
from jax.experimental.pallas import tpu as pltpu
from jax.sharding import PartitionSpec as P

HEAD_DIM = 128
F32 = jnp.float32
BF16 = jnp.bfloat16


NZ, NX = 9, 7
EDGE_QKV = {0: ((1, 2),), 2: ((1, 3),), 3: ((2, 2),), 5: ((2, 3),), 6: ((3, 1),), 7: ((3, 2),), 9: ((3, 3),)}
EDGE_W = {10: (1,), 11: (2,), 12: (3,), 14: (4,), 15: (5,)}
EDGE_W_OUT = {0: (1, 2), 1: (3,), 2: (4,), 3: (5,), 4: (6,), 5: (7, 8)}
EDGE_W_TAIL = ((), (6,), (7, 8))
MID_QKV = {0: ((1, 2),), 2: ((2, 2),), 3: ((3, 3),), 4: ((1, 3),), 6: ((2, 3),)}
MID_W_EARLY = {3: (1,), 4: (2,), 5: (3,), 6: (4,), 7: (5,), 8: (6,), 9: (7, 8)}
MID_W = {8: (1,), 9: (2,), 10: (3,), 11: (4,), 12: (5,), 13: (6,), 14: (7, 8)}
EDGE_W_FREE = {11: (0,), 12: (1, 2), 13: (3,), 14: (4,), 15: (5,)}
MID_W_FREE = {8: (0,), 9: (1,), 10: (2, 3), 11: (4,), 12: (5, 6), 13: (7, 8)}
V_EDGE_OPEN = {1: (0,)}
V_MID_OPEN = {3: (0,)}
V_MID_FAR = {4: (0,)}
V_MID_NEAR = {8: (0,)}
V_EDGE = {10: (0,)}
V_FINISH = {12: (0,)}
VMEM_MIB = 48
NQ = 2
COMM = True
COMP = True


def fused(S, H, NS, tokens, bank, slots, w_query, w_key, w_value, w_out, out,
          G, WO, VB, tok, normed, rows_in, qb, att, acc,
          ld_sem, wl_sem, zr, xr, send_n, send_f, send_x,
          wzr, wxr, wsend_r, wsend_l, wsend_x, turn_s, turn_r, turn_l,
          hq_s, hq_r, ha_s, ha_r, att_s, att_y, att_m, att_b,
          vt_s, vt_r, vt_l, vz_s, vz_r, vx_s, vx_r, vy_s, vy_r):
    s, h, b = lax.axis_index("seq"), lax.axis_index("head"), lax.axis_index("batch")
    nblk, nrow, D = bank.shape
    T = tokens.shape[0]
    blk = T // nblk
    CW = HEAD_DIM
    RS = w_query.shape[0]
    RH = RS // 2
    KH = H * CW // 2
    KQ = KH // 2
    NW = 2 * NS
    units = NS
    per = nblk // units
    GR = per * blk

    def dev(seq, head, batch):
        return {"seq": seq, "head": head, "batch": batch}

    def rcopy(src, dst, ss, rs, device):
        return pltpu.make_async_remote_copy(
            src_ref=src, dst_ref=dst, send_sem=ss, recv_sem=rs,
            device_id=device, device_id_type=pl.DeviceIdType.MESH)

    edge = jnp.logical_or(s == 0, s == S - 1)
    middle = jnp.logical_and(s > 0, s < S - 1)
    near_dev = (s - 1) * 3
    far_dev = 3 - s
    edge_dev = 1 + s // 3
    side = lax.rem(h, 2)
    mate = (h // 2) * 2 + 1 - side
    across = lax.rem(h + 2, H)
    peers = (mate, across, lax.rem(mate + 2, H))

    w_loads = []
    for j in range(NS):
        for k, w in enumerate((w_query, w_key, w_value)):
            c = pltpu.make_async_copy(
                w.at[:, pl.ds(j * CW, CW)],
                G.at[j, pl.ds(s * RS, RS), pl.ds(k * CW, CW)], wl_sem.at[j])
            w_loads.append(c)
    for c in w_loads[:3]:
        c.start()
    wo_own = pltpu.make_async_copy(w_out, WO.at[:, pl.ds(h * CW, CW), :], turn_l)

    tok_load = pltpu.make_async_copy(tokens, tok, ld_sem.at[1])
    bank_loads = [pltpu.make_async_copy(bank.at[i], rows_in.at[i], ld_sem.at[0]) for i in range(nblk)]

    barrier = pltpu.get_barrier_semaphore()

    def greet(device):
        pl.semaphore_signal(barrier, inc=1, device_id=device, device_id_type=pl.DeviceIdType.MESH)

    for p in peers:
        greet(dev(s, p, b))
    greet(dev(s, h, 1 - b))

    @pl.when(edge)
    def _():
        greet(dev(edge_dev, h, b))
        pl.semaphore_wait(barrier, 5)

    @pl.when(middle)
    def _():
        greet(dev(near_dev, h, b))
        greet(dev(far_dev, h, b))
        pl.semaphore_wait(barrier, 6)

    RQ = RH // NQ

    def chunk(t, origin, half, q):
        return G.at[t, pl.ds(origin * RS + half * RH + q * RQ, RQ), :]

    def near(t, origin, q):
        return rcopy(chunk(t, origin, b, q), chunk(t, origin, b, q), send_n, zr.at[t, origin, q],
                     dev(near_dev, h, b))

    def far(t, origin, q):
        return rcopy(chunk(t, origin, b, q), chunk(t, origin, b, q), send_f, zr.at[t, origin, q],
                     dev(far_dev, h, b))

    def inward(t, origin, q):
        return rcopy(chunk(t, origin, b, q), chunk(t, origin, b, q), send_n, zr.at[t, origin, q],
                     dev(edge_dev, h, b))

    def twin(t, origin, q):
        return rcopy(chunk(t, origin, b, q), chunk(t, origin, b, q), send_x, xr.at[t], dev(s, h, 1 - b))

    def send_own(way, t):
        for q in range(NQ):
            way(t, s, q).start()

    def edge_event(t, d):
        o = d + (s // 3) * (3 - 2 * d)
        for q in range(NQ):
            inward(t, o, q).wait_recv()
            twin(t, o, q).start()

    def forward(way, t, o, q):
        way(t, o, q).wait_recv()
        way(t, o, q).start()
        twin(t, o, q).start()

    def mid_first(t):
        a, e = 3 - s, 3 * (s - 1)
        if t == 0:
            for q in range(NQ):
                forward(near, t, a, q)
                forward(far, t, e, q)
        else:
            for q in range(NQ):
                forward(far, t, e, q)
            for q in range(NQ):
                forward(near, t, a, q)

    def mid_second(t):
        for q in range(NQ):
            forward(near, t, 3 * (2 - s), q)

    def turn(j, device):
        return rcopy(w_out, WO.at[:, pl.ds(j * CW, CW), :], turn_s, turn_r, device)

    def wpart(k, half):
        return WO.at[k // 2, pl.ds(half * KH + (k % 2) * KQ, KQ), :]

    def wpiece(k):
        return wpart(k, b) if k < NW else wpart(2 * NW - 1 - k, 1 - b)

    def wright(k):
        return rcopy(wpiece(k), wpiece(k), wsend_r, wzr.at[k], dev(lax.rem(s + 1, S), h, b))

    def wleft(k):
        return rcopy(wpiece(k), wpiece(k), wsend_l, wzr.at[k], dev(lax.rem(s + S - 1, S), h, b))

    def wtwin(k, half):
        return rcopy(wpart(k, half), wpart(k, half), wsend_x, wxr.at[k // (NX - 1)], dev(s, h, 1 - b))

    def crowded(who):
        return jnp.logical_or(jnp.logical_and(who < H // 2, s > who), jnp.logical_and(who >= H // 2, s < who))

    crowd = crowded(h)
    carries = crowded(across)
    opens = s == across
    carrier = lax.rem(s + 2, H)

    def vturn(j, device):
        return rcopy(w_out.at[0], VB.at[j // 2], vt_s, vt_r, device)

    def vturn_here():
        return pltpu.make_async_copy(w_out.at[0], VB.at[h // 2], vt_l)

    def vz(k):
        return rcopy(VB.at[b], VB.at[b], vz_s, vz_r,
                     dev(lax.rem(s + S + 1 - 2 * (across // 2), S), h, b))

    def vx(k):
        return rcopy(VB.at[b], VB.at[b], vx_s, vx_r, dev(s, h, 1 - b))

    def vy(k, half):
        return rcopy(VB.at[half], WO.at[0, pl.ds(half * KH, KQ), :], vy_s, vy_r, dev(s, across, b))

    def v_open():
        @pl.when(opens)
        def _():
            @pl.when(side == 0)
            def _():
                vturn_here().wait()
                rcopy(VB.at[0], VB.at[0], vt_s, vt_r, dev(s, mate, b)).wait_recv()

            @pl.when(side == 1)
            def _():
                rcopy(VB, VB, vt_s, vt_r, dev(s, mate, b)).wait_recv()
            vz(0).start()

    onward = jnp.logical_or(jnp.logical_and(across < H // 2, s < S - 1), jnp.logical_and(across >= H // 2, s > 0))

    def v_relay(k):
        @pl.when(carries)
        def _():
            vz(k).wait_recv()

            @pl.when(onward)
            def _():
                vz(k).start()
            vx(k).start()
            vy(k, b).start()

    def v_finish():
        @pl.when(carries)
        def _():
            rcopy(VB.at[0], VB.at[0], vx_s, vx_r, dev(s, h, 1 - b)).wait_recv()
            vy(0, 1 - b).start()

    def wo_turned():
        wo_own.wait()
        three = WO.at[:, pl.ds(0, (H - 1) * CW), :]
        rcopy(three, three, turn_s, turn_r, dev(s, mate, b)).wait_recv()

    def wo_out(rightward, k):
        @pl.when(jnp.logical_and(rightward, s < S - 1))
        def _():
            wright(k).start()

        @pl.when(jnp.logical_and(jnp.logical_not(rightward), s > 0))
        def _():
            wleft(k).start()

    def wrelay(k):
        wright(k).wait_recv()

        @pl.when(jnp.logical_and(s > h, s < S - 1))
        def _():
            wright(k).start()

        @pl.when(jnp.logical_and(s < h, s > 0))
        def _():
            wleft(k).start()
        if k < NX:
            wtwin(k, b).start()

    def ask(t):
        return rcopy(qb.at[t, pl.ds(0, blk), :], qb.at[t, pl.ds(T, blk), :], hq_s, hq_r.at[t],
                     dev(lax.rem(s + S - 1, S), h, b))

    def answer(t):
        return rcopy(att.at[t, h, pl.ds(T, blk), :], att.at[t, h, pl.ds(0, blk), :], ha_s, ha_r.at[t],
                     dev(lax.rem(s + 1, S), h, b))

    def att_rows(t, who, g):
        return att.at[t, who, pl.ds(blk + g * GR, GR), :]

    def att_copy(t, g, who, rs, device):
        return rcopy(att_rows(t, who, g), att_rows(t, who, g), att_s, rs, dev(s, device, b))

    def att_send(t, g):
        att_copy(t, g, h, att_m.at[0, t], mate).start()
        att_copy(t, g, h, att_y.at[t, g], across).start()

    def att_pass(t, g):
        att_copy(t, g, across, att_y.at[t, g], across).wait_recv()
        att_copy(t, g, across, att_m.at[1, t], mate).start()

    def att_got(t):
        for k in range(2):
            block = att.at[t, 0, pl.ds(blk, T), :]
            rcopy(block, block, att_s, att_m.at[k, t], dev(s, mate, b)).wait_recv()

    def att_first(t, k, who, device):
        part = att.at[t, who, pl.ds(0, blk), :]
        return rcopy(part, part, att_s, att_b.at[k, t // (NS - 1)], dev(s, device, b))

    def first_out(t):
        @pl.when(s > 0)
        def _():
            answer(t).wait_recv()
            for k in range(3):
                att_first(t, k, h, peers[k]).start()

    def first_got(i, n):
        @pl.when(s > 0)
        def _():
            for k in range(3):
                part = att.at[0:n, 0, pl.ds(0, blk), :]
                rcopy(part, part, att_s, att_b.at[k, i], dev(s, peers[k], b)).wait_recv()

    scale = math.log2(math.e) / math.sqrt(HEAD_DIM)

    def attend_all(blocks):
        scores = []
        for t, c, kv in blocks:
            q = qb[t, pl.ds(c * blk, blk), :]
            scores.append(lax.dot_general(q, kv[:, :CW], (((1,), (1,)), ((), ())), preferred_element_type=F32))
        for (t, c, kv), sc in zip(blocks, scores):
            e = jnp.exp2((sc - jnp.max(sc, axis=-1, keepdims=True)) * scale)
            p = (e * (1.0 / jnp.sum(e, axis=-1, keepdims=True))).astype(BF16)
            o = jnp.dot(p, kv[:, CW:], preferred_element_type=F32)
            att[t, h, pl.ds(c * blk, blk), :] = o.astype(BF16)

    def project(t, rows):
        return jnp.dot(rows, G[t, :, pl.ds(CW, 2 * CW)], preferred_element_type=F32).astype(BF16)

    def unit(t, g):
        first = 1 + g * per
        rows = [rows_in[slots[first + i - 1]] for i in range(per)]
        kv = project(t, jnp.concatenate(rows, axis=0))
        attend_all([(t, first + i, kv[i * nrow:(i + 1) * nrow]) for i in range(per)])

    def queries(t):
        qb[t, pl.ds(0, T), :] = jnp.dot(normed[...], G[t, :, pl.ds(0, CW)], preferred_element_type=F32).astype(BF16)

    def loaded(j):
        own = G.at[j, pl.ds(s * RS, RS), :]
        pltpu.make_async_copy(own, own, wl_sem.at[j]).wait()

    loaded(0)
    for c in w_loads[3:]:
        c.start()
    if COMM:
        @pl.when(middle)
        def _():
            send_own(near, 0)
            send_own(far, 0)

        @pl.when(edge)
        def _():
            send_own(inward, 0)
    loaded(1)
    tok_load.start()

    @pl.when(h == s)
    def _():
        wo_own.start()
    for c in bank_loads:
        c.start()
    if COMM:
        @pl.when(middle)
        def _():
            send_own(near, 1)

        @pl.when(edge)
        def _():
            send_own(inward, 1)

        @pl.when(h != s)
        def _():
            turn(h, dev(s, s, b)).start()

        @pl.when(jnp.logical_and(opens, side == 0))
        def _():
            vturn_here().start()

        @pl.when(jnp.logical_and(jnp.logical_not(opens), side == 0))
        def _():
            vturn(h, dev(s, carrier, b)).start()
    loaded(2)
    loaded(3)
    if COMM:
        @pl.when(edge)
        def _():
            send_own(inward, 2)
            send_own(inward, 3)

            edge_event(0, 1)

        @pl.when(middle)
        def _():
            mid_first(0)
            send_own(far, 1)
    tok_load.wait()

    def norm(i, _):
        x = tok[pl.ds(i * blk, blk), :].astype(F32)
        normed[pl.ds(i * blk, blk), :] = (
            x * lax.rsqrt(jnp.mean(x * x, axis=-1, keepdims=True) + 1e-06)).astype(BF16)
        return 0
    if COMP:
        lax.fori_loop(0, nblk, norm, 0)

    pltpu.make_async_copy(bank, rows_in, ld_sem.at[0]).wait()
    if COMM:
        @pl.when(s == S - 1)
        def _():
            qb[:, pl.ds(T, blk), :] = jnp.zeros((NS, blk, CW), BF16)

        @pl.when(s == 0)
        def _():
            att[:, :, pl.ds(0, blk), :] = jnp.zeros((NS, H, blk, CW), BF16)

        @pl.when(edge)
        def _():
            for t, d in ((1, 1), (0, 2), (0, 3), (2, 1)):
                edge_event(t, d)

            @pl.when(h == s)
            def _():
                wo_turned()

        @pl.when(middle)
        def _():
            mid_second(0)
            send_own(near, 2)
            mid_first(1)
            send_own(far, 2)
            mid_second(1)

    def plan(n, table, event):
        t, g = n
        for at, items in table.items():
            if at % units == g:
                @pl.when(t == at // units)
                def _():
                    for item in items:
                        event(item)

    def events(n):
        @pl.when(edge)
        def _():
            plan(n, EDGE_QKV, lambda e: edge_event(*e))
            plan(n, V_EDGE_OPEN, lambda e: v_open())

            @pl.when(crowd)
            def _():
                plan(n, EDGE_W, wrelay)

            @pl.when(h == s)
            def _():
                plan(n, EDGE_W_OUT, lambda k: wo_out(s == 0, k))

            @pl.when(jnp.logical_not(jnp.logical_or(crowd, h == s)))
            def _():
                plan(n, EDGE_W_FREE, wrelay)
            plan(n, V_EDGE, v_relay)

        @pl.when(middle)
        def _():
            plan(n, MID_QKV, lambda e: mid_step(*e))

            @pl.when(h == s)
            def _():
                plan(n, {2: (0,)}, lambda k: wo_turned())
                plan(n, MID_W_EARLY, lambda k: wo_out(s == 1, k))
                plan(n, MID_W_FREE, lambda k: wo_out(s == 2, k))
            plan(n, V_MID_OPEN, lambda e: v_open())

            @pl.when(across == near_dev)
            def _():
                plan(n, V_MID_FAR, v_relay)

            @pl.when(across != near_dev)
            def _():
                plan(n, V_MID_NEAR, v_relay)

            @pl.when(h == near_dev)
            def _():
                plan(n, MID_W_EARLY, wrelay)

            @pl.when(jnp.logical_and(h != near_dev, h != s))
            def _():
                plan(n, MID_W, wrelay)
        plan(n, V_FINISH, lambda e: v_finish())

    def mid_step(kind, t):
        if kind == 1:
            mid_first(t)
            if t < NS - 1:
                send_own(far, t + 1)
        elif kind == 2:
            mid_second(t)
        else:
            send_own(near, t)

    def slot(n, _):
        t, g = n // units, lax.rem(n, units)
        u = g + (s // 2) * (((g + 1) // 2) * (1 - g // 2) * 2 - g // 2)
        asked = jnp.logical_and(u == units - 1, s < S - 1)

        @pl.when(g == 0)
        def _():
            if COMM:
                twin_span = G.at[t, pl.ds(0, (S - 1) * RH), :]
                rcopy(twin_span, twin_span, send_x, xr.at[t], dev(s, h, 1 - b)).wait_recv()
            if COMP:
                queries(t)
            if COMM:
                @pl.when(s > 0)
                def _():
                    ask(t).start()
        if COMM:
            @pl.when(asked)
            def _():
                ask(t).wait_recv()
        if COMP:
            unit(t, u)
        if COMM:
            att_send(t, u)

            @pl.when(asked)
            def _():
                answer(t).start()
            for i in range(units):
                @pl.when(g == i)
                def _():
                    events((t, i))

            @pl.when(t > 0)
            def _():
                att_pass(t - 1, u)

                @pl.when(g == units - 1)
                def _():
                    first_out(t - 1)
        return 0

    lax.fori_loop(0, NS * units, slot, 0)

    def edge_w(ks):
        @pl.when(jnp.logical_and(edge, h != s))
        def _():
            for k in ks:
                wrelay(k)

    def wrows(n):
        return WO.at[:, pl.ds(0, n * KQ // NS), :]

    def wx_wait(i, n):
        rcopy(wrows(n), wrows(n), wsend_x, wxr.at[i], dev(s, h, 1 - b)).wait_recv()

    def wx_got(i, n):
        if i == 0:
            @pl.when(crowd)
            def _():
                wx_wait(i, n - 1)
                rcopy(VB, VB, vy_s, vy_r, dev(s, across, b)).wait_recv()

            @pl.when(jnp.logical_not(jnp.logical_or(crowd, h == s)))
            def _():
                wx_wait(i, n)
        else:
            @pl.when(h != s)
            def _():
                wx_wait(i, n)

    def gathered(ts, rows):
        return jnp.concatenate([att[t, k, rows, :] for t in ts for k in range(H)], axis=1)

    early = range(NS - 1)

    def fold_early(g, _):
        r = pl.ds(g * GR, GR)
        acc[r, :] = jnp.dot(gathered(early, r), WO[0:NS - 1].reshape((NS - 1) * H * CW, -1),
                            preferred_element_type=F32)
        return 0

    if COMM:
        edge_w(EDGE_W_TAIL[0])
        for g in range(units):
            att_pass(NS - 1, g)
        first_out(NS - 1)
        for t in early:
            att_got(t)
        first_got(0, NS - 1)
        edge_w(EDGE_W_TAIL[1])
        wx_got(0, NX - 1)
    if COMP:
        lax.fori_loop(0, units, fold_early, 0)
    if COMM:
        att_got(NS - 1)
        first_got(1, 1)
        edge_w(EDGE_W_TAIL[2])
        wx_got(1, 1)

    def fold_late(g, _):
        r = pl.ds(g * GR, GR)
        if COMP:
            part = jnp.dot(gathered((NS - 1,), r), WO[NS - 1], preferred_element_type=F32)
            out[r, :] = (acc[r, :] + part).astype(BF16)
        return 0
    lax.fori_loop(0, units, fold_late, 0)

    def drained(span, sem, device):
        rcopy(span, span, sem, turn_r, device).wait_send()

    if COMM:
        beside = dev(s, mate, b)

        @pl.when(edge)
        def _():
            drained(G.at[:, pl.ds(0, RH), :], send_n, beside)

        @pl.when(middle)
        def _():
            drained(G.at[:, pl.ds(0, 3 * RH), :], send_n, beside)
            drained(G.at[:, pl.ds(0, 2 * RH), :], send_f, beside)
        drained(G.at[:, pl.ds(0, (S - 1) * RH), :], send_x, beside)
        drained(att.at[:, 0:3, pl.ds(0, T)], att_s, beside)
        firsts = att.at[:, 0, pl.ds(0, blk), :]

        @pl.when(s > 0)
        def _():
            drained(att.at[:, 0:3, pl.ds(0, blk)], att_s, beside)
            drained(firsts, hq_s, beside)

        @pl.when(s < S - 1)
        def _():
            drained(firsts, ha_s, beside)

        down = h >= H // 2

        @pl.when(jnp.logical_and(s >= h, s < S - 1))
        def _():
            @pl.when(down)
            def _():
                drained(wrows(NZ), wsend_r, beside)

            @pl.when(jnp.logical_not(down))
            def _():
                drained(wrows(NZ - 1), wsend_r, beside)

        @pl.when(jnp.logical_and(s <= h, s > 0))
        def _():
            @pl.when(down)
            def _():
                drained(wrows(NZ - 1), wsend_l, beside)

            @pl.when(jnp.logical_not(down))
            def _():
                drained(wrows(NZ), wsend_l, beside)

        @pl.when(crowd)
        def _():
            drained(wrows(NX - 1), wsend_x, beside)

        @pl.when(jnp.logical_not(jnp.logical_or(crowd, h == s)))
        def _():
            drained(wrows(NX), wsend_x, beside)

        @pl.when(h != s)
        def _():
            drained(w_out, turn_s, beside)

        @pl.when(jnp.logical_and(jnp.logical_not(opens), side == 0))
        def _():
            drained(VB.at[0], vt_s, beside)

        @pl.when(jnp.logical_or(opens, jnp.logical_and(carries, onward)))
        def _():
            drained(VB.at[0], vz_s, beside)

        @pl.when(carries)
        def _():
            drained(VB.at[0], vx_s, beside)
            drained(VB, vy_s, beside)
    else:
        @pl.when(h == s)
        def _():
            wo_own.wait()


def one_kernel(tokens, neighbor_bank, slots, w_query, w_key, w_value, w_out):
    S, H = lax.axis_size("seq"), lax.axis_size("head")
    T, D = tokens.shape
    nblk, nrow = neighbor_bank.shape[:2]
    width = w_query.shape[1]
    NS = width // HEAD_DIM
    blk = T // nblk
    CW = HEAD_DIM
    out_cols = D // H
    dma = pltpu.SemaphoreType.DMA
    hbm = pl.BlockSpec(memory_space=pltpu.HBM)
    tokens, neighbor_bank, slots, w_query, w_key, w_value, w_out = [
        pltpu.with_memory_space_constraint(x, pltpu.HBM)
        for x in (tokens, neighbor_bank, slots, w_query, w_key, w_value, w_out.reshape(NS, CW, -1))]
    return pl.pallas_call(
        functools.partial(fused, S, H, NS),
        out_shape=jax.ShapeDtypeStruct((T, out_cols), BF16),
        in_specs=[hbm, hbm, pl.BlockSpec(memory_space=pltpu.SMEM), hbm, hbm, hbm, hbm],
        out_specs=pl.BlockSpec(memory_space=pltpu.VMEM),
        scratch_shapes=[
            pltpu.VMEM((NS, D, 3 * CW), BF16),
            pltpu.VMEM((NS, H * CW, out_cols), BF16),
            pltpu.VMEM((2, CW, out_cols), BF16),
            pltpu.VMEM((T, D), BF16),
            pltpu.VMEM((T, D), BF16),
            pltpu.VMEM((nblk, nrow, D), BF16),
            pltpu.VMEM((NS, T + blk, CW), BF16),
            pltpu.VMEM((NS, H, T + blk, CW), BF16),
            pltpu.VMEM((T, out_cols), F32),
            dma((2,)),
            dma((NS,)),
            dma((NS, S, NQ)), dma((NS,)), dma, dma, dma,
            dma((NZ,)), dma((2,)), dma, dma, dma, dma, dma, dma,
            dma, dma((NS,)), dma, dma((NS,)),
            dma, dma((NS, NS)), dma((2, NS)), dma((3, 2)),
            dma, dma, dma, dma, dma, dma, dma, dma, dma,
        ],
        compiler_params=pltpu.CompilerParams(
            collective_id=0, has_side_effects=True, vmem_limit_bytes=VMEM_MIB * 1024 * 1024),
    )(tokens, neighbor_bank, slots, w_query, w_key, w_value, w_out)


def passed_along(block, axis, distance):
    devices = range(lax.axis_size(axis))
    route = [(i - distance, i) for i in devices if i - distance in devices]
    return lax.ppermute(block, axis, route)


def attend(query_blocks, key_blocks, value_blocks):
    scores = jnp.einsum(
        "cmhd,cnhd->chmn", query_blocks, key_blocks, preferred_element_type=jnp.float32
    ) / math.sqrt(HEAD_DIM)
    peak_score = jnp.max(scores, axis=-1, keepdims=True)
    exponent = jnp.exp(scores - peak_score)
    weights = (exponent / jnp.sum(exponent, axis=-1, keepdims=True)).astype(jnp.bfloat16)
    blended = jnp.einsum(
        "chmn,cnhd->cmhd", weights, value_blocks, preferred_element_type=jnp.float32
    ).astype(jnp.bfloat16)
    return blended.reshape(blended.shape[0] * blended.shape[1], blended.shape[2] * blended.shape[3])


def fold_rows(source, shard_rows):
    return jnp.dot(source, shard_rows, preferred_element_type=jnp.float32)


def local(tokens, neighbor_bank, slots, w_query, w_key, w_value, w_out):
    tok_rows, model_width = tokens.shape
    block_count = neighbor_bank.shape[0]
    neighbor_rows = neighbor_bank.shape[1]
    block_len = tok_rows // block_count
    local_width = w_query.shape[1]
    local_heads = local_width // HEAD_DIM
    hidden = tokens.astype(jnp.float32)
    normed = (hidden * lax.rsqrt(jnp.mean(hidden * hidden, axis=-1, keepdims=True) + 1e-06)).astype(
        jnp.bfloat16
    )
    retrieved = jnp.take(neighbor_bank, slots, axis=0)
    arrived = passed_along(retrieved[block_count - 1], "seq", 1)
    context = jnp.concatenate([arrived[None], retrieved[: block_count - 1]], axis=0)
    context_flat = context.reshape(block_count * neighbor_rows, model_width)
    query_sum = fold_rows(normed, lax.all_gather(w_query, "seq", axis=0, tiled=True))
    key_sum = fold_rows(context_flat, lax.all_gather(w_key, "seq", axis=0, tiled=True))
    value_sum = fold_rows(context_flat, lax.all_gather(w_value, "seq", axis=0, tiled=True))
    query_blocks = query_sum.astype(jnp.bfloat16).reshape(
        block_count, block_len, local_heads, HEAD_DIM
    )
    key_blocks = key_sum.astype(jnp.bfloat16).reshape(
        block_count, neighbor_rows, local_heads, HEAD_DIM
    )
    value_blocks = value_sum.astype(jnp.bfloat16).reshape(
        block_count, neighbor_rows, local_heads, HEAD_DIM
    )
    attended = attend(query_blocks, key_blocks, value_blocks)
    every_head = lax.all_gather(attended, "head", axis=1, tiled=True)
    wide_rows = lax.all_gather(w_out, "seq", axis=1, tiled=True)
    own_columns = lax.all_to_all(wide_rows, "head", split_axis=1, concat_axis=0, tiled=True)
    return jnp.dot(every_head, own_columns, preferred_element_type=jnp.float32).astype(jnp.bfloat16)


def solution(mesh):
    in_specs = (
        P(("batch", "seq"), None),
        P(("batch", "seq"), None, None),
        P(("batch", "seq")),
        P("seq", "head"),
        P("seq", "head"),
        P("seq", "head"),
        P("head", "seq"),
    )
    out_specs = P(("batch", "seq"), "head")
    square = mesh.shape["seq"] == 4 and mesh.shape["head"] == 4 and mesh.shape["batch"] == 2
    body = one_kernel if square else local
    return jax.shard_map(body, mesh=mesh, in_specs=in_specs, out_specs=out_specs, check_vma=False)
```

```python
import functools
import math

import jax
import jax.numpy as jnp
from jax import lax
from jax.experimental import pallas as pl
from jax.experimental.pallas import tpu as pltpu
from jax.sharding import PartitionSpec as P

HEAD_DIM = 128
F32 = jnp.float32
BF16 = jnp.bfloat16


NZ, NX = 9, 7
EDGE_QKV = {0: ((1, 2),), 2: ((1, 3),), 3: ((2, 2),), 5: ((2, 3),), 6: ((3, 1),), 7: ((3, 2),), 9: ((3, 3),)}
EDGE_W = {10: (1,), 11: (2,), 12: (3,), 14: (4,), 15: (5,)}
EDGE_W_OUT = {0: (1, 2), 1: (3,), 2: (4,), 3: (5,), 4: (6,), 5: (7, 8)}
EDGE_W_TAIL = ((), (6,), (7, 8))
MID_QKV = {0: ((1, 2),), 2: ((2, 2),), 3: ((3, 3),), 4: ((1, 3),), 6: ((2, 3),)}
MID_W_EARLY = {3: (1,), 4: (2,), 5: (3,), 6: (4,), 7: (5,), 8: (6,), 9: (7, 8)}
MID_W = {8: (1,), 9: (2,), 10: (3,), 11: (4,), 12: (5,), 13: (6,), 14: (7, 8)}
EDGE_W_FREE = {11: (0,), 12: (1, 2), 13: (3,), 14: (4,), 15: (5,)}
MID_W_FREE = {8: (0,), 9: (1,), 10: (2, 3), 11: (4,), 12: (5, 6), 13: (7, 8)}
V_EDGE_OPEN = {1: (0,)}
V_MID_OPEN = {3: (0,)}
V_MID_FAR = {4: (0,)}
V_MID_NEAR = {7: (0,)}
V_EDGE = {10: (0,)}
V_FINISH = {12: (0,)}
VMEM_MIB = 48
NQ = 2
COMM = True
COMP = True


def fused(S, H, NS, tokens, bank, slots, w_query, w_key, w_value, w_out, out,
          G, WO, VB, tok, normed, rows_in, qb, att, acc,
          ld_sem, wl_sem, zr, xr, send_n, send_f, send_x,
          wzr, wxr, wsend_r, wsend_l, wsend_x, turn_s, turn_r, turn_l,
          hq_s, hq_r, ha_s, ha_r, att_s, att_y, att_m, att_b,
          vt_s, vt_r, vt_l, vz_s, vz_r, vx_s, vx_r, vy_s, vy_r):
    s, h, b = lax.axis_index("seq"), lax.axis_index("head"), lax.axis_index("batch")
    nblk, nrow, D = bank.shape
    T = tokens.shape[0]
    blk = T // nblk
    CW = HEAD_DIM
    RS = w_query.shape[0]
    RH = RS // 2
    KH = H * CW // 2
    KQ = KH // 2
    NW = 2 * NS
    units = NS
    per = nblk // units
    GR = per * blk

    def dev(seq, head, batch):
        return {"seq": seq, "head": head, "batch": batch}

    def rcopy(src, dst, ss, rs, device):
        return pltpu.make_async_remote_copy(
            src_ref=src, dst_ref=dst, send_sem=ss, recv_sem=rs,
            device_id=device, device_id_type=pl.DeviceIdType.MESH)

    edge = jnp.logical_or(s == 0, s == S - 1)
    middle = jnp.logical_and(s > 0, s < S - 1)
    near_dev = (s - 1) * 3
    far_dev = 3 - s
    edge_dev = 1 + s // 3
    side = lax.rem(h, 2)
    mate = (h // 2) * 2 + 1 - side
    across = lax.rem(h + 2, H)
    peers = (mate, across, lax.rem(mate + 2, H))

    w_loads = []
    for j in range(NS):
        for k, w in enumerate((w_query, w_key, w_value)):
            c = pltpu.make_async_copy(
                w.at[:, pl.ds(j * CW, CW)],
                G.at[j, pl.ds(s * RS, RS), pl.ds(k * CW, CW)], wl_sem.at[j])
            w_loads.append(c)
    for c in w_loads[:3]:
        c.start()
    wo_own = pltpu.make_async_copy(w_out, WO.at[:, pl.ds(h * CW, CW), :], turn_l)

    tok_load = pltpu.make_async_copy(tokens, tok, ld_sem.at[1])
    bank_loads = [pltpu.make_async_copy(bank.at[i], rows_in.at[i], ld_sem.at[0]) for i in range(nblk)]

    barrier = pltpu.get_barrier_semaphore()

    def greet(device):
        pl.semaphore_signal(barrier, inc=1, device_id=device, device_id_type=pl.DeviceIdType.MESH)

    for p in peers:
        greet(dev(s, p, b))
    greet(dev(s, h, 1 - b))

    @pl.when(edge)
    def _():
        greet(dev(edge_dev, h, b))
        pl.semaphore_wait(barrier, 5)

    @pl.when(middle)
    def _():
        greet(dev(near_dev, h, b))
        greet(dev(far_dev, h, b))
        pl.semaphore_wait(barrier, 6)

    RQ = RH // NQ

    def chunk(t, origin, half, q):
        return G.at[t, pl.ds(origin * RS + half * RH + q * RQ, RQ), :]

    def near(t, origin, q):
        return rcopy(chunk(t, origin, b, q), chunk(t, origin, b, q), send_n, zr.at[t, origin, q],
                     dev(near_dev, h, b))

    def far(t, origin, q):
        return rcopy(chunk(t, origin, b, q), chunk(t, origin, b, q), send_f, zr.at[t, origin, q],
                     dev(far_dev, h, b))

    def inward(t, origin, q):
        return rcopy(chunk(t, origin, b, q), chunk(t, origin, b, q), send_n, zr.at[t, origin, q],
                     dev(edge_dev, h, b))

    def twin(t, origin, q):
        return rcopy(chunk(t, origin, b, q), chunk(t, origin, b, q), send_x, xr.at[t], dev(s, h, 1 - b))

    def send_own(way, t):
        for q in range(NQ):
            way(t, s, q).start()

    def edge_event(t, d):
        o = d + (s // 3) * (3 - 2 * d)
        for q in range(NQ):
            inward(t, o, q).wait_recv()
            twin(t, o, q).start()

    def forward(way, t, o, q):
        way(t, o, q).wait_recv()
        way(t, o, q).start()
        twin(t, o, q).start()

    def mid_first(t):
        a, e = 3 - s, 3 * (s - 1)
        if t == 0:
            for q in range(NQ):
                forward(near, t, a, q)
                forward(far, t, e, q)
        else:
            for q in range(NQ):
                forward(far, t, e, q)
            for q in range(NQ):
                forward(near, t, a, q)

    def mid_second(t):
        for q in range(NQ):
            forward(near, t, 3 * (2 - s), q)

    def turn(j, device):
        return rcopy(w_out, WO.at[:, pl.ds(j * CW, CW), :], turn_s, turn_r, device)

    def wpart(k, half):
        return WO.at[k // 2, pl.ds(half * KH + (k % 2) * KQ, KQ), :]

    def wpiece(k):
        return wpart(k, b) if k < NW else wpart(2 * NW - 1 - k, 1 - b)

    def wright(k):
        return rcopy(wpiece(k), wpiece(k), wsend_r, wzr.at[k], dev(lax.rem(s + 1, S), h, b))

    def wleft(k):
        return rcopy(wpiece(k), wpiece(k), wsend_l, wzr.at[k], dev(lax.rem(s + S - 1, S), h, b))

    def wtwin(k, half):
        return rcopy(wpart(k, half), wpart(k, half), wsend_x, wxr.at[k // 2], dev(s, h, 1 - b))

    def crowded(who):
        return jnp.logical_or(jnp.logical_and(who < H // 2, s > who), jnp.logical_and(who >= H // 2, s < who))

    crowd = crowded(h)
    carries = crowded(across)
    opens = s == across
    carrier = lax.rem(s + 2, H)

    def vturn(j, device):
        return rcopy(w_out.at[0], VB.at[j // 2], vt_s, vt_r, device)

    def vturn_here():
        return pltpu.make_async_copy(w_out.at[0], VB.at[h // 2], vt_l)

    def vz(k):
        return rcopy(VB.at[b], VB.at[b], vz_s, vz_r,
                     dev(lax.rem(s + S + 1 - 2 * (across // 2), S), h, b))

    def vx(k):
        return rcopy(VB.at[b], VB.at[b], vx_s, vx_r, dev(s, h, 1 - b))

    def vy(k, half):
        return rcopy(VB.at[half], WO.at[0, pl.ds(half * KH, KQ), :], vy_s, vy_r, dev(s, across, b))

    def v_open():
        @pl.when(opens)
        def _():
            @pl.when(side == 0)
            def _():
                vturn_here().wait()
                rcopy(VB.at[0], VB.at[0], vt_s, vt_r, dev(s, mate, b)).wait_recv()

            @pl.when(side == 1)
            def _():
                rcopy(VB, VB, vt_s, vt_r, dev(s, mate, b)).wait_recv()
            vz(0).start()

    onward = jnp.logical_or(jnp.logical_and(across < H // 2, s < S - 1), jnp.logical_and(across >= H // 2, s > 0))

    def v_relay(k):
        @pl.when(carries)
        def _():
            vz(k).wait_recv()

            @pl.when(onward)
            def _():
                vz(k).start()
            vx(k).start()
            vy(k, b).start()

    def v_finish():
        @pl.when(carries)
        def _():
            rcopy(VB.at[0], VB.at[0], vx_s, vx_r, dev(s, h, 1 - b)).wait_recv()
            vy(0, 1 - b).start()

    def wo_turned():
        wo_own.wait()
        three = WO.at[:, pl.ds(0, (H - 1) * CW), :]
        rcopy(three, three, turn_s, turn_r, dev(s, mate, b)).wait_recv()

    def wo_out(rightward, k):
        @pl.when(jnp.logical_and(rightward, s < S - 1))
        def _():
            wright(k).start()

        @pl.when(jnp.logical_and(jnp.logical_not(rightward), s > 0))
        def _():
            wleft(k).start()

    def wrelay(k):
        wright(k).wait_recv()

        @pl.when(jnp.logical_and(s > h, s < S - 1))
        def _():
            wright(k).start()

        @pl.when(jnp.logical_and(s < h, s > 0))
        def _():
            wleft(k).start()
        if k < NX:
            wtwin(k, b).start()

    def ask(t):
        return rcopy(qb.at[t, pl.ds(0, blk), :], qb.at[t, pl.ds(T, blk), :], hq_s, hq_r.at[t],
                     dev(lax.rem(s + S - 1, S), h, b))

    def answer(t):
        return rcopy(att.at[t, h, pl.ds(T, blk), :], att.at[t, h, pl.ds(0, blk), :], ha_s, ha_r.at[t],
                     dev(lax.rem(s + 1, S), h, b))

    def att_rows(t, who, g):
        return att.at[t, who, pl.ds(blk + g * GR, GR), :]

    def att_copy(t, g, who, rs, device):
        return rcopy(att_rows(t, who, g), att_rows(t, who, g), att_s, rs, dev(s, device, b))

    def att_send(t, g):
        att_copy(t, g, h, att_m.at[0, t], mate).start()
        att_copy(t, g, h, att_y.at[t, g], across).start()

    def att_pass(t, g):
        att_copy(t, g, across, att_y.at[t, g], across).wait_recv()
        att_copy(t, g, across, att_m.at[1, t], mate).start()

    def att_got(t):
        for k in range(2):
            block = att.at[t, 0, pl.ds(blk, T), :]
            rcopy(block, block, att_s, att_m.at[k, t], dev(s, mate, b)).wait_recv()

    def att_first(t, k, who, device):
        part = att.at[t, who, pl.ds(0, blk), :]
        return rcopy(part, part, att_s, att_b.at[k, t], dev(s, device, b))

    def first_out(t):
        @pl.when(s > 0)
        def _():
            answer(t).wait_recv()
            for k in range(3):
                att_first(t, k, h, peers[k]).start()

    def first_got(i, n):
        @pl.when(s > 0)
        def _():
            for k in range(3):
                part = att.at[0:n, 0, pl.ds(0, blk), :]
                rcopy(part, part, att_s, att_b.at[k, i], dev(s, peers[k], b)).wait_recv()

    scale = math.log2(math.e) / math.sqrt(HEAD_DIM)

    def attend_all(blocks):
        scores = []
        for t, c, kv in blocks:
            q = qb[t, pl.ds(c * blk, blk), :]
            scores.append(lax.dot_general(q, kv[:, :CW], (((1,), (1,)), ((), ())), preferred_element_type=F32))
        for (t, c, kv), sc in zip(blocks, scores):
            e = jnp.exp2((sc - jnp.max(sc, axis=-1, keepdims=True)) * scale)
            p = (e * (1.0 / jnp.sum(e, axis=-1, keepdims=True))).astype(BF16)
            o = jnp.dot(p, kv[:, CW:], preferred_element_type=F32)
            att[t, h, pl.ds(c * blk, blk), :] = o.astype(BF16)

    def project(t, rows):
        return jnp.dot(rows, G[t, :, pl.ds(CW, 2 * CW)], preferred_element_type=F32).astype(BF16)

    def unit(t, g):
        first = 1 + g * per
        rows = [rows_in[slots[first + i - 1]] for i in range(per)]
        kv = project(t, jnp.concatenate(rows, axis=0))
        attend_all([(t, first + i, kv[i * nrow:(i + 1) * nrow]) for i in range(per)])

    def queries(t):
        qb[t, pl.ds(0, T), :] = jnp.dot(normed[...], G[t, :, pl.ds(0, CW)], preferred_element_type=F32).astype(BF16)

    def loaded(j):
        own = G.at[j, pl.ds(s * RS, RS), :]
        pltpu.make_async_copy(own, own, wl_sem.at[j]).wait()

    loaded(0)
    for c in w_loads[3:]:
        c.start()
    if COMM:
        @pl.when(middle)
        def _():
            send_own(near, 0)
            send_own(far, 0)

        @pl.when(edge)
        def _():
            send_own(inward, 0)
    loaded(1)
    tok_load.start()

    @pl.when(h == s)
    def _():
        wo_own.start()
    for c in bank_loads:
        c.start()
    if COMM:
        @pl.when(middle)
        def _():
            send_own(near, 1)

        @pl.when(edge)
        def _():
            send_own(inward, 1)

        @pl.when(h != s)
        def _():
            turn(h, dev(s, s, b)).start()

        @pl.when(jnp.logical_and(opens, side == 0))
        def _():
            vturn_here().start()

        @pl.when(jnp.logical_and(jnp.logical_not(opens), side == 0))
        def _():
            vturn(h, dev(s, carrier, b)).start()
    loaded(2)
    loaded(3)
    if COMM:
        @pl.when(edge)
        def _():
            send_own(inward, 2)
            send_own(inward, 3)

            edge_event(0, 1)

        @pl.when(middle)
        def _():
            mid_first(0)
            send_own(far, 1)
    tok_load.wait()

    def norm(i, _):
        x = tok[pl.ds(i * blk, blk), :].astype(F32)
        normed[pl.ds(i * blk, blk), :] = (
            x * lax.rsqrt(jnp.mean(x * x, axis=-1, keepdims=True) + 1e-06)).astype(BF16)
        return 0
    if COMP:
        lax.fori_loop(0, nblk, norm, 0)

    pltpu.make_async_copy(bank, rows_in, ld_sem.at[0]).wait()
    if COMM:
        @pl.when(s == S - 1)
        def _():
            qb[:, pl.ds(T, blk), :] = jnp.zeros((NS, blk, CW), BF16)

        @pl.when(s == 0)
        def _():
            att[:, :, pl.ds(0, blk), :] = jnp.zeros((NS, H, blk, CW), BF16)

        @pl.when(edge)
        def _():
            for t, d in ((1, 1), (0, 2), (0, 3), (2, 1)):
                edge_event(t, d)

            @pl.when(h == s)
            def _():
                wo_turned()

        @pl.when(middle)
        def _():
            mid_second(0)
            send_own(near, 2)
            mid_first(1)
            send_own(far, 2)
            mid_second(1)

    def plan(n, table, event):
        t, g = n
        for at, items in table.items():
            if at % units == g:
                @pl.when(t == at // units)
                def _():
                    for item in items:
                        event(item)

    def events(n):
        @pl.when(edge)
        def _():
            plan(n, EDGE_QKV, lambda e: edge_event(*e))
            plan(n, V_EDGE_OPEN, lambda e: v_open())

            @pl.when(crowd)
            def _():
                plan(n, EDGE_W, wrelay)

            @pl.when(h == s)
            def _():
                plan(n, EDGE_W_OUT, lambda k: wo_out(s == 0, k))

            @pl.when(jnp.logical_not(jnp.logical_or(crowd, h == s)))
            def _():
                plan(n, EDGE_W_FREE, wrelay)
            plan(n, V_EDGE, v_relay)

        @pl.when(middle)
        def _():
            plan(n, MID_QKV, lambda e: mid_step(*e))

            @pl.when(h == s)
            def _():
                plan(n, {2: (0,)}, lambda k: wo_turned())
                plan(n, MID_W_EARLY, lambda k: wo_out(s == 1, k))
                plan(n, MID_W_FREE, lambda k: wo_out(s == 2, k))
            plan(n, V_MID_OPEN, lambda e: v_open())

            @pl.when(across == near_dev)
            def _():
                plan(n, V_MID_FAR, v_relay)

            @pl.when(across != near_dev)
            def _():
                plan(n, V_MID_NEAR, v_relay)

            @pl.when(h == near_dev)
            def _():
                plan(n, MID_W_EARLY, wrelay)

            @pl.when(jnp.logical_and(h != near_dev, h != s))
            def _():
                plan(n, MID_W, wrelay)
        plan(n, V_FINISH, lambda e: v_finish())

    def mid_step(kind, t):
        if kind == 1:
            mid_first(t)
            if t < NS - 1:
                send_own(far, t + 1)
        elif kind == 2:
            mid_second(t)
        else:
            send_own(near, t)

    def slot(n, _):
        t, g = n // units, lax.rem(n, units)
        u = g + (s // 2) * (((g + 1) // 2) * (1 - g // 2) * 2 - g // 2)
        asked = jnp.logical_and(u == units - 1, s < S - 1)

        @pl.when(g == 0)
        def _():
            if COMM:
                twin_span = G.at[t, pl.ds(0, (S - 1) * RH), :]
                rcopy(twin_span, twin_span, send_x, xr.at[t], dev(s, h, 1 - b)).wait_recv()
            if COMP:
                queries(t)
            if COMM:
                @pl.when(s > 0)
                def _():
                    ask(t).start()
        if COMM:
            @pl.when(asked)
            def _():
                ask(t).wait_recv()
        if COMP:
            unit(t, u)
        if COMM:
            att_send(t, u)

            @pl.when(asked)
            def _():
                answer(t).start()
            for i in range(units):
                @pl.when(g == i)
                def _():
                    events((t, i))

            @pl.when(t > 0)
            def _():
                att_pass(t - 1, u)

                @pl.when(g == units - 1)
                def _():
                    first_out(t - 1)
        return 0

    lax.fori_loop(0, NS * units, slot, 0)

    def edge_w(ks):
        @pl.when(jnp.logical_and(edge, h != s))
        def _():
            for k in ks:
                wrelay(k)

    def wrows(n):
        return WO.at[:, pl.ds(0, n * KQ // NS), :]

    def wx_wait(i, n):
        rcopy(wrows(n), wrows(n), wsend_x, wxr.at[i], dev(s, h, 1 - b)).wait_recv()

    def wx_got(i, n):
        if i == 0:
            @pl.when(crowd)
            def _():
                wx_wait(i, n - 1)
                rcopy(VB, VB, vy_s, vy_r, dev(s, across, b)).wait_recv()

            @pl.when(jnp.logical_not(jnp.logical_or(crowd, h == s)))
            def _():
                wx_wait(i, n)
        else:
            @pl.when(h != s)
            def _():
                wx_wait(i, n)

    def gathered(ts, rows):
        return jnp.concatenate([att[t, k, rows, :] for t in ts for k in range(H)], axis=1)

    early = (0, 1)

    def fold_early(g, _):
        r = pl.ds(g * GR, GR)
        acc[r, :] = jnp.dot(gathered(early, r), WO[0:2].reshape(2 * H * CW, -1), preferred_element_type=F32)
        return 0

    if COMM:
        for g in range(2):
            att_pass(NS - 1, g)
        for t in early:
            att_got(t)
            first_got(t, 1)
            wx_got(t, 2)
    if COMP:
        lax.fori_loop(0, units, fold_early, 0)
    if COMM:
        edge_w(EDGE_W_TAIL[1])
        for g in range(2, units):
            att_pass(NS - 1, g)
        first_out(NS - 1)
        att_got(2)
        first_got(2, 1)
        wx_got(2, 2)

    def fold_next(g, _):
        r = pl.ds(g * GR, GR)
        acc[r, :] += jnp.dot(gathered((2,), r), WO[2], preferred_element_type=F32)
        return 0
    if COMP:
        lax.fori_loop(0, units, fold_next, 0)
    if COMM:
        edge_w(EDGE_W_TAIL[2])
        att_got(NS - 1)
        first_got(NS - 1, 1)
        wx_got(NS - 1, 1)

    def fold_late(g, _):
        r = pl.ds(g * GR, GR)
        if COMP:
            part = jnp.dot(gathered((NS - 1,), r), WO[NS - 1], preferred_element_type=F32)
            out[r, :] = (acc[r, :] + part).astype(BF16)
        return 0
    lax.fori_loop(0, units, fold_late, 0)

    def drained(span, sem, device):
        rcopy(span, span, sem, turn_r, device).wait_send()

    if COMM:
        beside = dev(s, mate, b)

        @pl.when(edge)
        def _():
            drained(G.at[:, pl.ds(0, RH), :], send_n, beside)

        @pl.when(middle)
        def _():
            drained(G.at[:, pl.ds(0, 3 * RH), :], send_n, beside)
            drained(G.at[:, pl.ds(0, 2 * RH), :], send_f, beside)
        drained(G.at[:, pl.ds(0, (S - 1) * RH), :], send_x, beside)
        drained(att.at[:, 0:3, pl.ds(0, T)], att_s, beside)
        firsts = att.at[:, 0, pl.ds(0, blk), :]

        @pl.when(s > 0)
        def _():
            drained(att.at[:, 0:3, pl.ds(0, blk)], att_s, beside)
            drained(firsts, hq_s, beside)

        @pl.when(s < S - 1)
        def _():
            drained(firsts, ha_s, beside)

        down = h >= H // 2

        @pl.when(jnp.logical_and(s >= h, s < S - 1))
        def _():
            @pl.when(down)
            def _():
                drained(wrows(NZ), wsend_r, beside)

            @pl.when(jnp.logical_not(down))
            def _():
                drained(wrows(NZ - 1), wsend_r, beside)

        @pl.when(jnp.logical_and(s <= h, s > 0))
        def _():
            @pl.when(down)
            def _():
                drained(wrows(NZ - 1), wsend_l, beside)

            @pl.when(jnp.logical_not(down))
            def _():
                drained(wrows(NZ), wsend_l, beside)

        @pl.when(crowd)
        def _():
            drained(wrows(NX - 1), wsend_x, beside)

        @pl.when(jnp.logical_not(jnp.logical_or(crowd, h == s)))
        def _():
            drained(wrows(NX), wsend_x, beside)

        @pl.when(h != s)
        def _():
            drained(w_out, turn_s, beside)

        @pl.when(jnp.logical_and(jnp.logical_not(opens), side == 0))
        def _():
            drained(VB.at[0], vt_s, beside)

        @pl.when(jnp.logical_or(opens, jnp.logical_and(carries, onward)))
        def _():
            drained(VB.at[0], vz_s, beside)

        @pl.when(carries)
        def _():
            drained(VB.at[0], vx_s, beside)
            drained(VB, vy_s, beside)
    else:
        @pl.when(h == s)
        def _():
            wo_own.wait()


def one_kernel(tokens, neighbor_bank, slots, w_query, w_key, w_value, w_out):
    S, H = lax.axis_size("seq"), lax.axis_size("head")
    T, D = tokens.shape
    nblk, nrow = neighbor_bank.shape[:2]
    width = w_query.shape[1]
    NS = width // HEAD_DIM
    blk = T // nblk
    CW = HEAD_DIM
    out_cols = D // H
    dma = pltpu.SemaphoreType.DMA
    hbm = pl.BlockSpec(memory_space=pltpu.HBM)
    tokens, neighbor_bank, slots, w_query, w_key, w_value, w_out = [
        pltpu.with_memory_space_constraint(x, pltpu.HBM)
        for x in (tokens, neighbor_bank, slots, w_query, w_key, w_value, w_out.reshape(NS, CW, -1))]
    return pl.pallas_call(
        functools.partial(fused, S, H, NS),
        out_shape=jax.ShapeDtypeStruct((T, out_cols), BF16),
        in_specs=[hbm, hbm, pl.BlockSpec(memory_space=pltpu.SMEM), hbm, hbm, hbm, hbm],
        out_specs=pl.BlockSpec(memory_space=pltpu.VMEM),
        scratch_shapes=[
            pltpu.VMEM((NS, D, 3 * CW), BF16),
            pltpu.VMEM((NS, H * CW, out_cols), BF16),
            pltpu.VMEM((2, CW, out_cols), BF16),
            pltpu.VMEM((T, D), BF16),
            pltpu.VMEM((T, D), BF16),
            pltpu.VMEM((nblk, nrow, D), BF16),
            pltpu.VMEM((NS, T + blk, CW), BF16),
            pltpu.VMEM((NS, H, T + blk, CW), BF16),
            pltpu.VMEM((T, out_cols), F32),
            dma((2,)),
            dma((NS,)),
            dma((NS, S, NQ)), dma((NS,)), dma, dma, dma,
            dma((NZ,)), dma((NS,)), dma, dma, dma, dma, dma, dma,
            dma, dma((NS,)), dma, dma((NS,)),
            dma, dma((NS, NS)), dma((2, NS)), dma((3, NS)),
            dma, dma, dma, dma, dma, dma, dma, dma, dma,
        ],
        compiler_params=pltpu.CompilerParams(
            collective_id=0, has_side_effects=True, vmem_limit_bytes=VMEM_MIB * 1024 * 1024),
    )(tokens, neighbor_bank, slots, w_query, w_key, w_value, w_out)


def passed_along(block, axis, distance):
    devices = range(lax.axis_size(axis))
    route = [(i - distance, i) for i in devices if i - distance in devices]
    return lax.ppermute(block, axis, route)


def attend(query_blocks, key_blocks, value_blocks):
    scores = jnp.einsum(
        "cmhd,cnhd->chmn", query_blocks, key_blocks, preferred_element_type=jnp.float32
    ) / math.sqrt(HEAD_DIM)
    peak_score = jnp.max(scores, axis=-1, keepdims=True)
    exponent = jnp.exp(scores - peak_score)
    weights = (exponent / jnp.sum(exponent, axis=-1, keepdims=True)).astype(jnp.bfloat16)
    blended = jnp.einsum(
        "chmn,cnhd->cmhd", weights, value_blocks, preferred_element_type=jnp.float32
    ).astype(jnp.bfloat16)
    return blended.reshape(blended.shape[0] * blended.shape[1], blended.shape[2] * blended.shape[3])


def fold_rows(source, shard_rows):
    return jnp.dot(source, shard_rows, preferred_element_type=jnp.float32)


def local(tokens, neighbor_bank, slots, w_query, w_key, w_value, w_out):
    tok_rows, model_width = tokens.shape
    block_count = neighbor_bank.shape[0]
    neighbor_rows = neighbor_bank.shape[1]
    block_len = tok_rows // block_count
    local_width = w_query.shape[1]
    local_heads = local_width // HEAD_DIM
    hidden = tokens.astype(jnp.float32)
    normed = (hidden * lax.rsqrt(jnp.mean(hidden * hidden, axis=-1, keepdims=True) + 1e-06)).astype(
        jnp.bfloat16
    )
    retrieved = jnp.take(neighbor_bank, slots, axis=0)
    arrived = passed_along(retrieved[block_count - 1], "seq", 1)
    context = jnp.concatenate([arrived[None], retrieved[: block_count - 1]], axis=0)
    context_flat = context.reshape(block_count * neighbor_rows, model_width)
    query_sum = fold_rows(normed, lax.all_gather(w_query, "seq", axis=0, tiled=True))
    key_sum = fold_rows(context_flat, lax.all_gather(w_key, "seq", axis=0, tiled=True))
    value_sum = fold_rows(context_flat, lax.all_gather(w_value, "seq", axis=0, tiled=True))
    query_blocks = query_sum.astype(jnp.bfloat16).reshape(
        block_count, block_len, local_heads, HEAD_DIM
    )
    key_blocks = key_sum.astype(jnp.bfloat16).reshape(
        block_count, neighbor_rows, local_heads, HEAD_DIM
    )
    value_blocks = value_sum.astype(jnp.bfloat16).reshape(
        block_count, neighbor_rows, local_heads, HEAD_DIM
    )
    attended = attend(query_blocks, key_blocks, value_blocks)
    every_head = lax.all_gather(attended, "head", axis=1, tiled=True)
    wide_rows = lax.all_gather(w_out, "seq", axis=1, tiled=True)
    own_columns = lax.all_to_all(wide_rows, "head", split_axis=1, concat_axis=0, tiled=True)
    return jnp.dot(every_head, own_columns, preferred_element_type=jnp.float32).astype(jnp.bfloat16)


def solution(mesh):
    in_specs = (
        P(("batch", "seq"), None),
        P(("batch", "seq"), None, None),
        P(("batch", "seq")),
        P("seq", "head"),
        P("seq", "head"),
        P("seq", "head"),
        P("head", "seq"),
    )
    out_specs = P(("batch", "seq"), "head")
    square = mesh.shape["seq"] == 4 and mesh.shape["head"] == 4 and mesh.shape["batch"] == 2
    body = one_kernel if square else local
    return jax.shard_map(body, mesh=mesh, in_specs=in_specs, out_specs=out_specs, check_vma=False)
```
